256 devices in a mesh: groups: 2 (over z), expert: 128 (over x, y, core).
Axes of the slice: x: 8, y: 8, z: 2, core: 2. Of those that a mesh axis runs over, the one named last changes fastest.
The devices are a block of a 8x8x16 slice.
Arguments:
- tokens: bfloat16 [1024, 6144], P(('groups', 'expert')), parts along dimension 0, may hold values from -64 to 64
- router_weight: bfloat16 [12288, 4], P('groups'), parts along dimension 0, may hold values from -1 to 1
- expert_ids: int32 [1024, 2], P(('groups', 'expert')), parts along dimension 0, may hold values from 0 to 3, as said below
- slots: int32 [1024, 2], P(('groups', 'expert')), parts along dimension 0, may hold values from 0 to 3, as said below
- gate_weight: bfloat16 [6144, 32768], P(None, 'expert'), may hold values from -0.078125 to 0.078125
- up_weight: bfloat16 [6144, 32768], P(None, 'expert'), may hold values from -0.078125 to 0.078125
- down_weight: bfloat16 [32768, 6144], P('expert'), may hold values from -0.0625 to 0.0625
Outputs:
- mixed_rows: bfloat16 [1024, 6144], P(('groups', 'expert')), parts along dimension 0
- balance: float32 [2], P('groups'), parts along dimension 0
The draws below stay inside these ranges and needn't reach their ends.
There are 2 independent parts, one for each index of `groups`. The reference program is written for one: setup_inputs(seed, part) draws one part's arguments, and reference() takes and returns one part's arrays. A program takes and returns all parts, laid end to end along the dimension named above; an argument that names none is the same for every part. Nothing has to cross between parts.
Inputs may be any that keep to these rules, and one draw needn't show every extreme that they name: `expert_ids`: each row names two different experts; one expert, drawn from the seed, is named by every token. Within the rows of one device the slots of the assignments to one expert are distinct; on every device exactly 2 assignments of the expert that every token names have slots below 2, and no expert has more.
All inputs are finite; a program needn't handle non-finite values.
Results may differ from the reference program's by a relative error of at most 0.0058.
Values may be sent and summed in bfloat16 or wider, within the bound.
No kernel may reach another device: no remote copies, remote signals or barrier semaphores. Data moves between devices by JAX's collectives and lax.ppermute only.
A program may use at most 64 MiB of HBM per device.

```python
import math
import jax
import jax.numpy as jnp
from jax import lax

D = 6144
FF_EXP = 8192
EXPERTS = 4
TOK_DEV = 4
CAP = 2
TOKENS = 512
FF_DEV = 256
N_EXPERT = 128


def route_ids(key):
    heavy = jax.random.randint(jax.random.fold_in(key, 11), (), 0, EXPERTS)
    offset = jax.random.randint(jax.random.fold_in(key, 12), (TOKENS,), 0, EXPERTS - 1)
    second_pick = (heavy + 1 + offset) % EXPERTS
    flipped = jax.random.randint(jax.random.fold_in(key, 13), (TOKENS,), 0, 2)
    first_col = jnp.where(flipped == 1, second_pick, heavy)
    second_col = jnp.where(flipped == 1, heavy, second_pick)
    return jnp.stack([first_col, second_col], axis=1).astype(jnp.int32)


def router_draw(key):
    values = jax.random.normal(jax.random.fold_in(key, 21), (D, EXPERTS), jnp.float32) / math.sqrt(D)
    return jnp.clip(values, -6.0 / math.sqrt(D), 6.0 / math.sqrt(D))


def draw_expert_ids(key, part):
    return route_ids(key)


def draw_router_weight(key, part):
    return router_draw(key).astype(jnp.bfloat16)


def draw_slots(key, part):
    routing = route_ids(key)
    blocks = TOKENS // TOK_DEV
    named = jnp.sum((routing[:, :, None] == jnp.arange(EXPERTS, dtype=jnp.int32)).astype(jnp.int32), axis=1)
    named = named.reshape(blocks, TOK_DEV, EXPERTS)
    ranking = jnp.clip(jnp.cumsum(named, axis=1) - 1, 0, TOK_DEV - 1)
    scores = jax.random.randint(jax.random.fold_in(key, 14), (blocks, EXPERTS, TOK_DEV), 0, 1 << 20)
    scores = scores * TOK_DEV + jnp.arange(TOK_DEV, dtype=jnp.int32)
    orders = jnp.argsort(scores, axis=2, stable=True).astype(jnp.int32)
    slot_table = jnp.take_along_axis(orders, jnp.transpose(ranking, (0, 2, 1)), axis=2)
    slot_table = jnp.transpose(slot_table, (0, 2, 1)).reshape(TOKENS, EXPERTS)
    return jnp.take_along_axis(slot_table, routing, axis=1).astype(jnp.int32)


def draw_tokens(key, part):
    row_pos = jnp.arange(TOKENS, dtype=jnp.float32)
    rising = jnp.exp(math.log(3.0) * row_pos / TOKENS)[:, None]
    row_scale = rising * jnp.exp(jax.random.uniform(jax.random.fold_in(key, 31), (TOKENS, 1), jnp.float32, math.log(0.7), math.log(1.4)))
    values = jax.random.normal(jax.random.fold_in(key, 32), (TOKENS, D), jnp.float32) * row_scale
    return jnp.clip(values, -64.0, 64.0).astype(jnp.bfloat16)


def block_scale(rng, dims, split, low, high):
    factor_of, own = 1.0, jax.random.fold_in(rng, 6)
    for position, blocks in split:
        heights = jnp.exp(jax.random.uniform(jax.random.fold_in(own, position), (blocks,), jnp.float32, low / len(split), high / len(split)))
        factor_of = factor_of * jnp.repeat(heights, dims[position] // blocks).reshape([-1 if axis == position else 1 for axis in range(len(dims))])
    return factor_of


def centred(stream_key, shape, scale, reach, cuts=(), kind=jnp.bfloat16):
    entries = jax.random.normal(stream_key, shape, jnp.float32) * scale
    if len(cuts) > 0:
        entries = block_scale(stream_key, shape, cuts, -0.22, 0.18) * entries
    return jnp.clip(entries, min=-reach, max=reach).astype(kind)


def setup_inputs(seed: int = 0, part: int = 0) -> dict:
    key_of = jax.random.split(jax.random.key(seed), 8)
    part_keys = jax.random.split(jax.random.fold_in(key_of[7], part), 8)
    tokens = draw_tokens(jax.random.fold_in(jax.random.fold_in(key_of[7], part), 71), part)
    router_weight = draw_router_weight(jax.random.fold_in(jax.random.fold_in(key_of[7], part), 71), part)
    expert_ids = draw_expert_ids(jax.random.fold_in(jax.random.fold_in(key_of[7], part), 71), part)
    slots = draw_slots(jax.random.fold_in(jax.random.fold_in(key_of[7], part), 71), part)
    gate_weight = centred(key_of[4], (D, EXPERTS * FF_EXP), D ** -0.5, 0.078125, ((1, 128),))
    up_weight = centred(key_of[5], (D, EXPERTS * FF_EXP), D ** -0.5, 0.078125, ((1, 128),))
    down_weight = centred(key_of[6], (EXPERTS * FF_EXP, D), FF_EXP ** -0.5, 0.0625, ((0, 128),))
    return {"tokens": tokens, "router_weight": router_weight, "expert_ids": expert_ids, "slots": slots, "gate_weight": gate_weight, "up_weight": up_weight, "down_weight": down_weight}


def expert_output(slot_rows, gate_weight, up_weight, down_weight, expert):
    group_size = N_EXPERT // EXPERTS

    def add_part(total, part_index):
        column = (expert * FF_EXP + part_index * FF_DEV).astype(jnp.int32)
        gate_cols = lax.dynamic_slice_in_dim(gate_weight, column, FF_DEV, 1)
        up_cols = lax.dynamic_slice_in_dim(up_weight, column, FF_DEV, 1)
        down_rows = lax.dynamic_slice_in_dim(down_weight, column, FF_DEV, 0)
        gate_pre = jnp.dot(slot_rows.astype(jnp.float32), gate_cols.astype(jnp.float32), preferred_element_type=jnp.float32)
        up_pre = jnp.dot(slot_rows.astype(jnp.float32), up_cols.astype(jnp.float32), preferred_element_type=jnp.float32)
        hidden = (jax.nn.silu(gate_pre) * up_pre).astype(jnp.bfloat16)
        partial_value = jnp.dot(hidden.astype(jnp.float32), down_rows.astype(jnp.float32), preferred_element_type=jnp.float32).astype(jnp.bfloat16)
        return (total + partial_value.astype(jnp.float32), None)
    start = jnp.zeros((slot_rows.shape[0], D), jnp.float32)
    total, unused = lax.scan(add_part, start, jnp.arange(group_size, dtype=jnp.int32))
    return total

def reference(tokens, router_weight, expert_ids, slots, gate_weight, up_weight, down_weight):
    blocks = TOKENS // TOK_DEV
    logits = jnp.dot(tokens.astype(jnp.float32), router_weight.astype(jnp.float32), preferred_element_type=jnp.float32)
    router_probs = jax.nn.softmax(logits, axis=1)
    chosen = jnp.take_along_axis(logits, expert_ids, axis=1)
    top_logit = jnp.max(chosen, axis=1, keepdims=True)
    raised = jnp.exp(chosen - top_logit)
    gate_values = raised / jnp.sum(raised, axis=1, keepdims=True)
    kept_gates = jnp.where(slots < CAP, gate_values, 0.0)
    named_onehot = (expert_ids[:, :, None] == jnp.arange(EXPERTS, dtype=jnp.int32)).astype(jnp.float32)
    counts = jnp.sum(named_onehot, axis=(0, 1))
    prob_sums = jnp.sum(router_probs, axis=0)
    balance = (EXPERTS * jnp.sum(counts / (2.0 * TOKENS) * (prob_sums / TOKENS))).reshape(1)
    slot_match = (slots[:, :, None, None] == jnp.arange(CAP, dtype=jnp.int32)).astype(jnp.float32)
    slot_onehot = named_onehot[:, :, :, None] * slot_match
    dispatch_map = jnp.sum(slot_onehot, axis=1).reshape(blocks, TOK_DEV, EXPERTS, CAP)
    combine_map = jnp.sum(slot_onehot * kept_gates[:, :, None, None], axis=1).reshape(blocks, TOK_DEV, EXPERTS, CAP)
    token_blocks = tokens.astype(jnp.float32).reshape(blocks, TOK_DEV, D)
    buffer = jnp.einsum('btec,btd->ebcd', dispatch_map, token_blocks, precision=lax.Precision.HIGHEST).astype(jnp.bfloat16)
    outputs = jnp.stack([expert_output(buffer[expert].reshape(blocks * CAP, D), gate_weight, up_weight, down_weight, expert).reshape(blocks, CAP, D) for expert in range(EXPERTS)])
    mixed_rows = jnp.einsum('btec,ebcd->btd', combine_map, outputs, precision=lax.Precision.HIGHEST)
    return (mixed_rows.reshape(TOKENS, D).astype(jnp.bfloat16), balance)
```

```python
import jax
import jax.numpy as jnp
from jax import lax
from jax.sharding import Mesh
from jax.sharding import PartitionSpec as P

EXPERTS = 4
CAP = 2
PAIR, RING, CORES = 2, 8, 2
EXPERT = ("xo", "xi", "y", "core")
GROUPS_EXPERT = ("groups",) + EXPERT


def shift(value, axis, size, step):
    return lax.ppermute(value, axis, [(i, (i + step) % size) for i in range(size)])


def swap(value, axis, size, bit):
    return lax.ppermute(value, axis, [(i, i ^ bit) for i in range(size)])


def local(tokens, router_weight, expert_ids, slots, gate_weight, up_weight, down_weight):
    devices = lax.axis_size(EXPERT)
    tok_rows, width = tokens.shape
    here = lax.axis_index("xo")
    expert_order = (here + jnp.arange(EXPERTS, dtype=jnp.int32)) % EXPERTS
    slot_iota = jnp.arange(CAP, dtype=jnp.int32)
    hit = (expert_ids[:, :, None, None] == expert_order[None, None, :, None]) & (
        slots[:, :, None, None] == slot_iota
    )
    select = jnp.any(hit, axis=1).reshape(tok_rows, EXPERTS * CAP)
    packed = jnp.dot(
        select.T.astype(jnp.bfloat16), tokens, preferred_element_type=jnp.float32
    ).astype(jnp.bfloat16)

    arrived = [packed[:CAP]]
    for k in range(1, EXPERTS):
        arrived.append(shift(packed[k * CAP : (k + 1) * CAP], "xo", EXPERTS, k))
    block_a = jnp.concatenate(arrived, axis=0)
    block_b = swap(block_a, "xi", PAIR, 1)

    half = RING // 2
    got = {(0, 0): block_a, (1, 0): block_b}
    for b, block in enumerate((block_a, block_b)):
        for sign in (1, -1):
            moving = block
            reach = half if (b == 0) == (sign == 1) else half - 1
            for d in range(1, reach + 1):
                moving = shift(moving, "y", RING, sign)
                got[(b, -sign * d)] = moving
    keys = sorted(got, key=lambda key: (-abs(key[1]), key[1], key[0]))
    mine = jnp.concatenate([got[key] for key in keys], axis=0)
    other = swap(mine, "core", CORES, 1)
    rows = jnp.concatenate([mine, other], axis=0)

    gate_pre = jnp.dot(rows, gate_weight, preferred_element_type=jnp.float32)
    up_pre = jnp.dot(rows, up_weight, preferred_element_type=jnp.float32)
    hidden = (jax.nn.silu(gate_pre) * up_pre).astype(jnp.bfloat16)
    partial = jnp.dot(hidden, down_weight, preferred_element_type=jnp.float32)

    count = mine.shape[0]
    from_other = swap(partial[count:].astype(jnp.bfloat16), "core", CORES, 1)
    summed = partial[:count] + from_other.astype(jnp.float32)
    size = EXPERTS * CAP
    part = {key: summed[i * size : (i + 1) * size] for i, key in enumerate(keys)}

    def back(b):
        total = part[(b, 0)]
        for sign in (1, -1):
            reach = half if (b == 0) == (sign == 1) else half - 1
            moving = None
            for d in range(reach, 0, -1):
                value = part[(b, -sign * d)]
                if moving is not None:
                    value = value + moving.astype(jnp.float32)
                moving = shift(value.astype(jnp.bfloat16), "y", RING, -sign)
            total = total + moving.astype(jnp.float32)
        return total

    total_b = back(1).astype(jnp.bfloat16)
    total_a = back(0) + swap(total_b, "xi", PAIR, 1).astype(jnp.float32)
    send = total_a.astype(jnp.bfloat16)
    returned = [total_a[:CAP]]
    for k in range(1, EXPERTS):
        returned.append(
            shift(send[k * CAP : (k + 1) * CAP], "xo", EXPERTS, -k).astype(jnp.float32)
        )
    expert_out = jnp.concatenate(returned, axis=0)

    logits = jnp.dot(tokens, router_weight, preferred_element_type=jnp.float32)
    router_probs = jax.nn.softmax(logits, axis=1)
    expert_iota = jnp.arange(EXPERTS, dtype=jnp.int32)
    named = (expert_ids[:, :, None] == expert_iota).astype(jnp.float32)
    chosen = jnp.sum(named * logits[:, None, :], axis=2)
    top_logit = jnp.max(chosen, axis=1, keepdims=True)
    raised = jnp.exp(chosen - top_logit)
    gate_values = raised / jnp.sum(raised, axis=1, keepdims=True)
    kept_gates = jnp.where(slots < CAP, gate_values, 0.0)
    combine = jnp.sum(hit * kept_gates[:, :, None, None], axis=1).reshape(
        tok_rows, EXPERTS * CAP
    )
    mixed_rows = jnp.dot(
        combine, expert_out, precision=lax.Precision.HIGHEST, preferred_element_type=jnp.float32
    ).astype(jnp.bfloat16)

    totals = jnp.stack([jnp.sum(named, axis=(0, 1)), jnp.sum(router_probs, axis=0)], axis=0)
    for axis, length in (("core", CORES), ("y", RING), ("xi", PAIR), ("xo", EXPERTS)):
        bit = 1
        while bit < length:
            totals = totals + swap(totals, axis, length, bit)
            bit *= 2
    total_tokens = tok_rows * devices
    balance = (
        EXPERTS * jnp.sum(totals[0] / (2.0 * total_tokens) * (totals[1] / total_tokens))
    ).reshape(1)
    return (mixed_rows, balance)


def solution(mesh):
    split = Mesh(
        mesh.devices.reshape(mesh.shape["groups"], EXPERTS, PAIR, RING, CORES),
        GROUPS_EXPERT,
    )
    placed = (
        P(GROUPS_EXPERT, None),
        P("groups", None),
        P(GROUPS_EXPERT, None),
        P(GROUPS_EXPERT, None),
        P(None, EXPERT),
        P(None, EXPERT),
        P(EXPERT, None),
    )
    return jax.shard_map(
        local,
        mesh=split,
        in_specs=placed,
        out_specs=(P(GROUPS_EXPERT, None), P("groups")),
        check_vma=False,
    )
```

```python
import jax
import jax.numpy as jnp
from jax import lax
from jax.experimental import pallas as pl
from jax.experimental.pallas import tpu as pltpu
from jax.sharding import Mesh
from jax.sharding import PartitionSpec as P

EXPERTS = 4
CAP = 2
PAIR, RING, CORES = 2, 8, 2
LANES = 128
EXPERT = ("xo", "xi", "y", "core")
GROUPS_EXPERT = ("groups",) + EXPERT
F32, BF16 = jnp.float32, jnp.bfloat16
HALF = RING // 2
BLOCKS = [(chunk, d) for d in range(1, HALF) for chunk in (0, 1)] + [(0, HALF)]


def vmem(count):
    return [pl.BlockSpec(memory_space=pltpu.VMEM)] * count


def call(kernel, outs, args, flops=200_000, in_specs=None):
    size = sum(a.size * a.dtype.itemsize for a in list(args) + list(outs))
    return pl.pallas_call(
        kernel,
        out_shape=outs,
        in_specs=in_specs or vmem(len(args)),
        out_specs=vmem(len(outs)),
        cost_estimate=pl.CostEstimate(flops=flops, bytes_accessed=size, transcendentals=0),
    )(*args)


def shape(rows, width, dtype):
    return jax.ShapeDtypeStruct((rows, width), dtype)


def pack_kernel(ids_s, slots_s, ids_v, slots_v, tok_ref, router_ref, own, s1, s2, s3, cw_ref):
    here = lax.axis_index("xo")
    count, width = tok_ref.shape
    tok = tok_ref[...].astype(F32)
    router = router_ref[...].astype(F32)
    ids = ids_v[...]
    slots = slots_v[...]
    logits = [
        jnp.sum(tok * router[e : e + 1, :], axis=1, keepdims=True) for e in range(EXPERTS)
    ]
    top = jnp.maximum(jnp.maximum(logits[0], logits[1]), jnp.maximum(logits[2], logits[3]))
    raised = [jnp.exp(v - top) for v in logits]
    inverse = 1.0 / (raised[0] + raised[1] + raised[2] + raised[3])
    lane = lax.broadcasted_iota(jnp.int32, (1, LANES), 1)
    count_row = jnp.zeros((1, LANES), F32)
    prob_row = jnp.zeros((1, LANES), F32)
    for e in range(EXPERTS):
        named = jnp.sum(
            jnp.sum((ids == e).astype(F32), axis=1, keepdims=True), axis=0, keepdims=True
        )
        prob = jnp.sum(raised[e] * inverse, axis=0, keepdims=True)
        high = prob.astype(BF16).astype(F32)
        count_row = jnp.where((lane == e) | (lane == e + EXPERTS), named, count_row)
        prob_row = jnp.where(lane == e, high, prob_row)
        prob_row = jnp.where(lane == e + EXPERTS, prob - high, prob_row)
    statistic = jnp.concatenate([count_row, prob_row], axis=0).astype(BF16)
    chosen = []
    for k in range(2):
        picked = jnp.zeros_like(logits[0])
        for e in range(EXPERTS):
            picked = jnp.where(ids[:, k : k + 1] == e, logits[e], picked)
        chosen.append(picked)
    top = jnp.maximum(chosen[0], chosen[1])
    chosen = [jnp.exp(v - top) for v in chosen]
    total = chosen[0] + chosen[1]
    gates = [v / total for v in chosen]
    lane = lax.broadcasted_iota(jnp.int32, (count, LANES), 1)
    weights = jnp.zeros((count, LANES), F32)
    for j, out in enumerate((own, s1, s2, s3)):
        expert = lax.rem(here + j, EXPERTS)
        rows = []
        for s in range(CAP):
            row = jnp.zeros((1, width), F32)
            for t in range(count):
                hit = ((ids_s[t, 0] == expert) & (slots_s[t, 0] == s)) | (
                    (ids_s[t, 1] == expert) & (slots_s[t, 1] == s)
                )
                row = jnp.where(hit, tok[t : t + 1, :], row)
            rows.append(row)
            column = jnp.zeros((count, 1), F32)
            for k in range(2):
                match = (ids[:, k : k + 1] == expert) & (slots[:, k : k + 1] == s)
                column = jnp.where(match, gates[k], column)
            weights = jnp.where(lane == j * CAP + s, column, weights)
        out[:, :width] = jnp.concatenate(rows, axis=0).astype(BF16)
        out[:, width:] = statistic
    cw_ref[...] = weights


def stack_kernel(a_ref, b_ref, out):
    rows = a_ref.shape[0]
    out[:rows, :] = a_ref[...]
    out[rows:, :] = b_ref[...]


def expert_kernel(scale, *refs):
    blocks = refs[:16]
    gate_ref, up_ref, down_ref = refs[16:19]
    outs = refs[19:35]
    balance_ref, hidden_ref = refs[35], refs[36]
    width = down_ref.shape[1]
    units = gate_ref.shape[1]
    rows = blocks[0].shape[0]
    tile = 256

    def step(i, carry):
        gate, up = carry
        at = pl.ds(pl.multiple_of(i * tile, tile), tile)
        x = jnp.concatenate([block[:, at] for block in blocks], axis=0)
        gate = gate + jnp.dot(x, gate_ref[at, :], preferred_element_type=F32)
        up = up + jnp.dot(x, up_ref[at, :], preferred_element_type=F32)
        return gate, up

    zero = jnp.zeros((16 * rows, units), F32)
    gate, up = lax.fori_loop(0, width // tile, step, (zero, zero))
    hidden_ref[...] = (gate * jax.nn.sigmoid(gate) * up).astype(BF16)

    def down(i, carry):
        at = pl.ds(pl.multiple_of(i * tile, tile), tile)
        value = jnp.dot(hidden_ref[...], down_ref[:, at], preferred_element_type=F32)
        for n, out in enumerate(outs):
            out[:, at] = value[n * rows : (n + 1) * rows, :].astype(out.dtype)
        return carry

    lax.fori_loop(0, width // tile, down, 0)

    total = jnp.zeros((rows, LANES), F32)
    for block in blocks:
        total = total + block[:, width:].astype(F32)
    parity = lax.broadcasted_iota(jnp.int32, total.shape, 0) % 2
    named = jnp.sum(jnp.where(parity == 0, total, 0.0), axis=0, keepdims=True)
    probs = jnp.sum(jnp.where(parity == 1, total, 0.0), axis=0, keepdims=True)
    balance_ref[...] = jnp.sum(named * probs, axis=1, keepdims=True) * scale


def add_kernel(*refs):
    value = refs[0][...]
    for ref in refs[1:-1]:
        value = value + ref[...].astype(F32)
    refs[-1][...] = value.astype(refs[-1].dtype)


def split_kernel(keep_ref, came_ref, a_ref, b_ref):
    rows = a_ref.shape[0]
    total = keep_ref[...] + came_ref[...].astype(F32)
    a_ref[...] = total[:rows]
    b_ref[...] = total[rows:].astype(BF16)


def part_kernel(a_ref, came_ref, own, s1, s2, s3):
    total = a_ref[...] + came_ref[...].astype(F32)
    for j, out in enumerate((own, s1, s2, s3)):
        out[...] = total[j * CAP : (j + 1) * CAP].astype(out.dtype)


def mix_kernel(cw_ref, own, r1, r2, r3, out):
    weights = cw_ref[...]
    total = None
    for j, ref in enumerate((own, r1, r2, r3)):
        value = ref[...].astype(F32)
        for s in range(CAP):
            at = j * CAP + s
            term = weights[:, at : at + 1] * value[s : s + 1, :]
            total = term if total is None else total + term
    out[...] = total.astype(out.dtype)


def to_expert(value, step):
    return lax.ppermute(value, "xo", [(i, (i + step) % EXPERTS) for i in range(EXPERTS)])


def swap(value, axis):
    return lax.ppermute(value, axis, [(0, 1), (1, 0)])


def ring(value, back):
    pairs = []
    for y in range(RING):
        for c in range(CORES):
            step = 1 if (c == 0) != back else -1
            pairs.append((y * CORES + c, (y + step) % RING * CORES + c))
    return lax.ppermute(value, ("y", "core"), pairs)


def local(tokens, router_weight, expert_ids, slots, gate_weight, up_weight, down_weight):
    devices = lax.axis_size(EXPERT)
    count, width = tokens.shape
    wide = width + LANES
    smem = pl.BlockSpec(memory_space=pltpu.SMEM)
    *sends, weights = call(
        pack_kernel,
        [shape(CAP, wide, BF16)] * EXPERTS + [shape(count, LANES, F32)],
        (expert_ids, slots, expert_ids, slots, tokens, router_weight.T),
        in_specs=[smem, smem] + vmem(4),
    )
    arrived = [sends[0]] + [to_expert(sends[k], k) for k in range(1, EXPERTS)]
    block = jnp.concatenate(arrived, axis=0)
    size = EXPERTS * CAP
    mine = call(stack_kernel, [shape(2 * size, wide, BF16)], (block, swap(block, "xi")))[0]
    theirs = swap(mine, "core")

    got = {}
    for chunk, start in ((0, mine), (1, theirs)):
        moving = start
        for d in range(1, HALF + 1 - chunk):
            moving = ring(moving, False)
            got[chunk, d] = moving
    near = [got[key] for key in BLOCKS]
    far = [swap(block, "core") for block in near]

    rows = 2 * size
    total_tokens = count * devices
    scale = EXPERTS / (2.0 * total_tokens * total_tokens)
    outs = pl.pallas_call(
        lambda *refs: expert_kernel(scale, *refs),
        out_shape=[shape(rows, width, F32)] * 9
        + [shape(rows, width, BF16)] * 7
        + [shape(1, 1, F32)],
        in_specs=vmem(19),
        out_specs=vmem(17),
        scratch_shapes=[pltpu.VMEM((16 * rows, gate_weight.shape[1]), BF16)],
        cost_estimate=pl.CostEstimate(
            flops=6 * 16 * rows * width * gate_weight.shape[1],
            bytes_accessed=18_000_000,
            transcendentals=0,
        ),
    )(mine, theirs, *near, *far, gate_weight, up_weight, down_weight)
    own_mine, own_theirs = outs[:2]
    kept = dict(zip(BLOCKS, outs[2:9]))
    crossed = {key: swap(value, "core") for key, value in reversed(list(zip(BLOCKS, outs[9:16])))}
    balance = outs[16].reshape(1)

    moving = {}
    for d in range(HALF, 0, -1):
        for chunk in (0, 1):
            if (chunk, d) in kept:
                terms = [kept[chunk, d], crossed[chunk, d]]
                if chunk in moving:
                    terms.append(moving[chunk])
                value = call(add_kernel, [shape(rows, width, BF16)], terms)[0]
                moving[chunk] = ring(value, True)
    cross = call(add_kernel, [shape(rows, width, BF16)], (own_theirs, moving[1]))[0]
    came = swap(cross, "core")
    keep = call(add_kernel, [shape(rows, width, F32)], (own_mine, moving[0]))[0]
    a_sum, b_sum = call(
        split_kernel, [shape(size, width, F32), shape(size, width, BF16)], (keep, came)
    )
    pieces = call(
        part_kernel,
        [shape(CAP, width, F32)] + [shape(CAP, width, BF16)] * 3,
        (a_sum, swap(b_sum, "xi")),
    )
    returned = [pieces[0]] + [to_expert(pieces[k], -k) for k in range(1, EXPERTS)]
    mixed_rows = call(mix_kernel, [shape(count, width, BF16)], (weights, *returned))[0]
    return (mixed_rows, balance)


def solution(mesh):
    split = Mesh(
        mesh.devices.reshape(mesh.shape["groups"], EXPERTS, PAIR, RING, CORES),
        GROUPS_EXPERT,
    )
    placed = (
        P(GROUPS_EXPERT, None),
        P("groups", None),
        P(GROUPS_EXPERT, None),
        P(GROUPS_EXPERT, None),
        P(None, EXPERT),
        P(None, EXPERT),
        P(EXPERT, None),
    )
    return jax.shard_map(
        local,
        mesh=split,
        in_specs=placed,
        out_specs=(P(GROUPS_EXPERT, None), P("groups")),
        check_vma=False,
    )
```

```python
import jax
import jax.numpy as jnp
from jax import lax
from jax.experimental import pallas as pl
from jax.experimental.pallas import tpu as pltpu
from jax.sharding import Mesh
from jax.sharding import PartitionSpec as P

EXPERTS = 4
CAP = 2
PAIR, RING, CORES = 2, 8, 2
LANES = 128
EXPERT = ("xo", "xi", "y", "core")
GROUPS_EXPERT = ("groups",) + EXPERT
F32, BF16 = jnp.float32, jnp.bfloat16
HALF = RING // 2
BLOCKS = [(chunk, d) for d in range(1, HALF) for chunk in (0, 1)] + [(0, HALF)]


def vmem(count):
    return [pl.BlockSpec(memory_space=pltpu.VMEM)] * count


def call(kernel, outs, args, flops=200_000, in_specs=None):
    size = sum(a.size * a.dtype.itemsize for a in list(args) + list(outs))
    return pl.pallas_call(
        kernel,
        out_shape=outs,
        in_specs=in_specs or vmem(len(args)),
        out_specs=vmem(len(outs)),
        cost_estimate=pl.CostEstimate(flops=flops, bytes_accessed=size, transcendentals=0),
        compiler_params=pltpu.CompilerParams(vmem_limit_bytes=4 << 20),
    )(*args)


def shape(rows, width, dtype):
    return jax.ShapeDtypeStruct((rows, width), dtype)


def pack_kernel(ids_s, slots_s, ids_v, slots_v, tok_ref, router_ref, own, s1, s2, s3, cw_ref):
    here = lax.axis_index("xo")
    count, width = tok_ref.shape
    tok = tok_ref[...].astype(F32)
    router = router_ref[...].astype(F32)
    ids = ids_v[...].T
    slots = slots_v[...].T
    logits = [
        jnp.sum(tok * router[e : e + 1, :], axis=1, keepdims=True) for e in range(EXPERTS)
    ]
    top = jnp.maximum(jnp.maximum(logits[0], logits[1]), jnp.maximum(logits[2], logits[3]))
    raised = [jnp.exp(v - top) for v in logits]
    inverse = 1.0 / (raised[0] + raised[1] + raised[2] + raised[3])
    lane = lax.broadcasted_iota(jnp.int32, (1, LANES), 1)
    count_row = jnp.zeros((1, LANES), F32)
    prob_row = jnp.zeros((1, LANES), F32)
    for e in range(EXPERTS):
        named = jnp.sum(
            jnp.sum((ids == e).astype(F32), axis=1, keepdims=True), axis=0, keepdims=True
        )
        prob = jnp.sum(raised[e] * inverse, axis=0, keepdims=True)
        high = prob.astype(BF16).astype(F32)
        count_row = jnp.where((lane == e) | (lane == e + EXPERTS), named, count_row)
        prob_row = jnp.where(lane == e, high, prob_row)
        prob_row = jnp.where(lane == e + EXPERTS, prob - high, prob_row)
    statistic = jnp.concatenate([count_row, prob_row], axis=0).astype(BF16)
    chosen = []
    for k in range(2):
        picked = jnp.zeros_like(logits[0])
        for e in range(EXPERTS):
            picked = jnp.where(ids[:, k : k + 1] == e, logits[e], picked)
        chosen.append(picked)
    top = jnp.maximum(chosen[0], chosen[1])
    chosen = [jnp.exp(v - top) for v in chosen]
    total = chosen[0] + chosen[1]
    gates = [v / total for v in chosen]
    lane = lax.broadcasted_iota(jnp.int32, (count, LANES), 1)
    weights = jnp.zeros((count, LANES), F32)
    for j, out in enumerate((own, s1, s2, s3)):
        expert = lax.rem(here + j, EXPERTS)
        rows = []
        for s in range(CAP):
            row = jnp.zeros((1, width), F32)
            for t in range(count):
                hit = ((ids_s[0, t] == expert) & (slots_s[0, t] == s)) | (
                    (ids_s[1, t] == expert) & (slots_s[1, t] == s)
                )
                row = jnp.where(hit, tok[t : t + 1, :], row)
            rows.append(row)
            column = jnp.zeros((count, 1), F32)
            for k in range(2):
                match = (ids[:, k : k + 1] == expert) & (slots[:, k : k + 1] == s)
                column = jnp.where(match, gates[k], column)
            weights = jnp.where(lane == j * CAP + s, column, weights)
        out[:, :width] = jnp.concatenate(rows, axis=0).astype(BF16)
        out[:, width:] = statistic
    cw_ref[...] = weights


def stack_kernel(a_ref, b_ref, out):
    rows = a_ref.shape[0]
    out[:rows, :] = a_ref[...]
    out[rows:, :] = b_ref[...]


def expert_kernel(scale, *refs):
    blocks = refs[:16]
    gate_ref, up_ref, down_ref = refs[16:19]
    outs = refs[19:35]
    balance_ref, hidden_ref = refs[35], refs[36]
    width = down_ref.shape[1]
    units = gate_ref.shape[1]
    rows = blocks[0].shape[0]
    tile = 256

    def step(i, carry):
        gate, up = carry
        at = pl.ds(pl.multiple_of(i * tile, tile), tile)
        x = jnp.concatenate([block[:, at] for block in blocks], axis=0)
        gate = gate + jnp.dot(x, gate_ref[at, :], preferred_element_type=F32)
        up = up + jnp.dot(x, up_ref[at, :], preferred_element_type=F32)
        return gate, up

    zero = jnp.zeros((16 * rows, units), F32)
    gate, up = lax.fori_loop(0, width // tile, step, (zero, zero))
    hidden_ref[...] = (gate * jax.nn.sigmoid(gate) * up).astype(BF16)

    def down(i, carry):
        at = pl.ds(pl.multiple_of(i * tile, tile), tile)
        value = jnp.dot(hidden_ref[...], down_ref[:, at], preferred_element_type=F32)
        for n, out in enumerate(outs):
            out[:, at] = value[n * rows : (n + 1) * rows, :].astype(out.dtype)
        return carry

    lax.fori_loop(0, width // tile, down, 0)

    total = jnp.zeros((rows, LANES), F32)
    for block in blocks:
        total = total + block[:, width:].astype(F32)
    parity = lax.broadcasted_iota(jnp.int32, total.shape, 0) % 2
    named = jnp.sum(jnp.where(parity == 0, total, 0.0), axis=0, keepdims=True)
    probs = jnp.sum(jnp.where(parity == 1, total, 0.0), axis=0, keepdims=True)
    balance_ref[...] = jnp.sum(named * probs, axis=1, keepdims=True) * scale


def add_kernel(*refs):
    value = refs[0][...]
    for ref in refs[1:-1]:
        value = value + ref[...].astype(F32)
    refs[-1][...] = value.astype(refs[-1].dtype)


def split_kernel(keep_ref, came_ref, a_ref, b_ref):
    rows = a_ref.shape[0]
    total = keep_ref[...] + came_ref[...].astype(F32)
    a_ref[...] = total[:rows]
    b_ref[...] = total[rows:].astype(BF16)


def part_kernel(a_ref, came_ref, own, s1, s2, s3):
    total = a_ref[...] + came_ref[...].astype(F32)
    for j, out in enumerate((own, s1, s2, s3)):
        out[...] = total[j * CAP : (j + 1) * CAP].astype(out.dtype)


def mix_kernel(cw_ref, own, r1, r2, r3, out):
    weights = cw_ref[...]
    total = None
    for j, ref in enumerate((own, r1, r2, r3)):
        value = ref[...].astype(F32)
        for s in range(CAP):
            at = j * CAP + s
            term = weights[:, at : at + 1] * value[s : s + 1, :]
            total = term if total is None else total + term
    out[...] = total.astype(out.dtype)


def to_expert(value, step):
    return lax.ppermute(value, "xo", [(i, (i + step) % EXPERTS) for i in range(EXPERTS)])


def swap(value, axis):
    return lax.ppermute(value, axis, [(0, 1), (1, 0)])


def ring(value, back):
    pairs = []
    for y in range(RING):
        for c in range(CORES):
            step = 1 if (c == 0) != back else -1
            pairs.append((y * CORES + c, (y + step) % RING * CORES + c))
    return lax.ppermute(value, ("y", "core"), pairs)


def local(tokens, router_weight, expert_ids, slots, gate_weight, up_weight, down_weight):
    devices = lax.axis_size(EXPERT)
    count, width = tokens.shape
    wide = width + LANES
    smem = pl.BlockSpec(memory_space=pltpu.SMEM)
    *sends, weights = call(
        pack_kernel,
        [shape(CAP, wide, BF16)] * EXPERTS + [shape(count, LANES, F32)],
        (expert_ids.T, slots.T, expert_ids.T, slots.T, tokens, router_weight.T),
        in_specs=[smem, smem] + vmem(4),
    )
    arrived = [sends[0]] + [to_expert(sends[k], k) for k in range(1, EXPERTS)]
    block = jnp.concatenate(arrived, axis=0)
    size = EXPERTS * CAP
    mine = call(stack_kernel, [shape(2 * size, wide, BF16)], (block, swap(block, "xi")))[0]
    theirs = swap(mine, "core")

    got = {}
    for chunk, start in ((0, mine), (1, theirs)):
        moving = start
        for d in range(1, HALF + 1 - chunk):
            moving = ring(moving, False)
            got[chunk, d] = moving
    near = [got[key] for key in BLOCKS]
    far = [swap(block, "core") for block in near]

    rows = 2 * size
    total_tokens = count * devices
    scale = EXPERTS / (2.0 * total_tokens * total_tokens)
    outs = pl.pallas_call(
        lambda *refs: expert_kernel(scale, *refs),
        out_shape=[shape(rows, width, F32)] * 9
        + [shape(rows, width, BF16)] * 7
        + [shape(1, 1, F32)],
        in_specs=vmem(19),
        out_specs=vmem(17),
        scratch_shapes=[pltpu.VMEM((16 * rows, gate_weight.shape[1]), BF16)],
        cost_estimate=pl.CostEstimate(
            flops=6 * 16 * rows * width * gate_weight.shape[1],
            bytes_accessed=18_000_000,
            transcendentals=0,
        ),
        compiler_params=pltpu.CompilerParams(vmem_limit_bytes=28 << 20),
    )(mine, theirs, *near, *far, gate_weight, up_weight, down_weight)
    own_mine, own_theirs = outs[:2]
    kept = dict(zip(BLOCKS, outs[2:9]))
    crossed = {key: swap(value, "core") for key, value in reversed(list(zip(BLOCKS, outs[9:16])))}
    balance = outs[16].reshape(1)

    moving = {}
    for d in range(HALF, 0, -1):
        for chunk in (0, 1):
            if (chunk, d) in kept:
                terms = [kept[chunk, d], crossed[chunk, d]]
                if chunk in moving:
                    terms.append(moving[chunk])
                value = call(add_kernel, [shape(rows, width, BF16)], terms)[0]
                moving[chunk] = ring(value, True)
    cross = call(add_kernel, [shape(rows, width, BF16)], (own_theirs, moving[1]))[0]
    came = swap(cross, "core")
    keep = call(add_kernel, [shape(rows, width, F32)], (own_mine, moving[0]))[0]
    a_sum, b_sum = call(
        split_kernel, [shape(size, width, F32), shape(size, width, BF16)], (keep, came)
    )
    pieces = call(
        part_kernel,
        [shape(CAP, width, F32)] + [shape(CAP, width, BF16)] * 3,
        (a_sum, swap(b_sum, "xi")),
    )
    returned = [pieces[0]] + [to_expert(pieces[k], -k) for k in range(1, EXPERTS)]
    mixed_rows = call(mix_kernel, [shape(count, width, BF16)], (weights, *returned))[0]
    return (mixed_rows, balance)


def solution(mesh):
    split = Mesh(
        mesh.devices.reshape(mesh.shape["groups"], EXPERTS, PAIR, RING, CORES),
        GROUPS_EXPERT,
    )
    placed = (
        P(GROUPS_EXPERT, None),
        P("groups", None),
        P(GROUPS_EXPERT, None),
        P(GROUPS_EXPERT, None),
        P(None, EXPERT),
        P(None, EXPERT),
        P(EXPERT, None),
    )
    return jax.shard_map(
        local,
        mesh=split,
        in_specs=placed,
        out_specs=(P(GROUPS_EXPERT, None), P("groups")),
        check_vma=False,
    )
```

```python
import jax
import jax.numpy as jnp
from jax import lax
from jax.experimental import pallas as pl
from jax.experimental.pallas import tpu as pltpu
from jax.sharding import Mesh
from jax.sharding import PartitionSpec as P

EXPERTS = 4
CAP = 2
PAIR, RING, CORES = 2, 8, 2
LANES = 128
EXPERT = ("xo", "xi", "y", "core")
GROUPS_EXPERT = ("groups",) + EXPERT
F32, BF16 = jnp.float32, jnp.bfloat16
HALF = RING // 2
BLOCKS = [(chunk, d) for d in range(1, HALF) for chunk in (0, 1)] + [(0, HALF)]


def vmem(count):
    return [pl.BlockSpec(memory_space=pltpu.VMEM)] * count


def call(kernel, outs, args, flops=200_000, in_specs=None, scratch=()):
    size = 1_000_000
    return pl.pallas_call(
        kernel,
        out_shape=outs,
        in_specs=in_specs or vmem(len(args)),
        out_specs=vmem(len(outs)),
        scratch_shapes=list(scratch),
        cost_estimate=pl.CostEstimate(flops=flops, bytes_accessed=size, transcendentals=0),
        compiler_params=pltpu.CompilerParams(vmem_limit_bytes=4 << 20),
    )(*args)


def shape(rows, width, dtype):
    return jax.ShapeDtypeStruct((rows, width), dtype)


def column_of(scalars, count):
    row = lax.broadcasted_iota(jnp.int32, (count, 1), 0)
    value = jnp.zeros((count, 1), jnp.int32)
    for t, scalar in enumerate(scalars):
        value = jnp.where(row == t, scalar, value)
    return value


def pack_kernel(
    ids_hbm,
    slots_hbm,
    tok_hbm,
    router_hbm,
    own,
    s1,
    s2,
    s3,
    cw_ref,
    tok_ref,
    router_ref,
    ids_s,
    slots_s,
    sems,
):
    copies = [
        pltpu.make_async_copy(tok_hbm, tok_ref, sems.at[0]),
        pltpu.make_async_copy(router_hbm, router_ref, sems.at[1]),
        pltpu.make_async_copy(ids_hbm, ids_s, sems.at[2]),
        pltpu.make_async_copy(slots_hbm, slots_s, sems.at[3]),
    ]
    for copy in copies:
        copy.start()
    here = lax.axis_index("xo")
    count, width = tok_ref.shape
    for copy in copies:
        copy.wait()
    ids = [column_of([ids_s[k, t] for t in range(count)], count) for k in range(2)]
    slots = [column_of([slots_s[k, t] for t in range(count)], count) for k in range(2)]
    tok = tok_ref[...].astype(F32)
    router = router_ref[...].astype(F32)
    logits = [
        jnp.sum(tok * router[e : e + 1, :], axis=1, keepdims=True) for e in range(EXPERTS)
    ]
    top = jnp.maximum(jnp.maximum(logits[0], logits[1]), jnp.maximum(logits[2], logits[3]))
    raised = [jnp.exp(v - top) for v in logits]
    inverse = 1.0 / (raised[0] + raised[1] + raised[2] + raised[3])
    lane = lax.broadcasted_iota(jnp.int32, (1, LANES), 1)
    count_row = jnp.zeros((1, LANES), F32)
    prob_row = jnp.zeros((1, LANES), F32)
    for e in range(EXPERTS):
        named = jnp.sum(
            (ids[0] == e).astype(F32) + (ids[1] == e).astype(F32), axis=0, keepdims=True
        )
        prob = jnp.sum(raised[e] * inverse, axis=0, keepdims=True)
        high = prob.astype(BF16).astype(F32)
        count_row = jnp.where((lane == e) | (lane == e + EXPERTS), named, count_row)
        prob_row = jnp.where(lane == e, high, prob_row)
        prob_row = jnp.where(lane == e + EXPERTS, prob - high, prob_row)
    statistic = jnp.concatenate([count_row, prob_row], axis=0).astype(BF16)
    chosen = []
    for k in range(2):
        picked = jnp.zeros_like(logits[0])
        for e in range(EXPERTS):
            picked = jnp.where(ids[k] == e, logits[e], picked)
        chosen.append(picked)
    top = jnp.maximum(chosen[0], chosen[1])
    chosen = [jnp.exp(v - top) for v in chosen]
    total = chosen[0] + chosen[1]
    gates = [v / total for v in chosen]
    lane = lax.broadcasted_iota(jnp.int32, (count, LANES), 1)
    weights = jnp.zeros((count, LANES), F32)
    for j, out in enumerate((own, s1, s2, s3)):
        expert = lax.rem(here + j, EXPERTS)
        rows = []
        for s in range(CAP):
            row = jnp.zeros((1, width), F32)
            for t in range(count):
                hit = ((ids_s[0, t] == expert) & (slots_s[0, t] == s)) | (
                    (ids_s[1, t] == expert) & (slots_s[1, t] == s)
                )
                row = jnp.where(hit, tok[t : t + 1, :], row)
            rows.append(row)
            column = jnp.zeros((count, 1), F32)
            for k in range(2):
                match = (ids[k] == expert) & (slots[k] == s)
                column = jnp.where(match, gates[k], column)
            weights = jnp.where(lane == j * CAP + s, column, weights)
        out[:, :width] = jnp.concatenate(rows, axis=0).astype(BF16)
        out[:, width:] = statistic
    cw_ref[...] = weights


def in_hbm(value):
    return pltpu.with_memory_space_constraint(value, pltpu.HBM)


def fetch_kernel(*refs):
    count = (len(refs) - 2) // 2
    copies = [
        pltpu.make_async_copy(refs[n], refs[count + 1 + n], refs[-1].at[n]) for n in range(count)
    ]
    for copy in copies:
        copy.start()
    for copy in copies:
        copy.wait()


def fetch(weights, after):
    anyway = pl.BlockSpec(memory_space=pl.ANY)
    return pl.pallas_call(
        fetch_kernel,
        out_shape=[pltpu.VMEM(w.shape, w.dtype) for w in weights],
        in_specs=[pl.BlockSpec(memory_space=pltpu.HBM)] * len(weights) + [anyway],
        out_specs=vmem(len(weights)),
        scratch_shapes=[pltpu.SemaphoreType.DMA((len(weights),))],
        cost_estimate=pl.CostEstimate(
            flops=1_000_000,
            bytes_accessed=sum(2 * w.size * w.dtype.itemsize for w in weights),
            transcendentals=0,
        ),
        compiler_params=pltpu.CompilerParams(vmem_limit_bytes=4 << 20),
    )(*[in_hbm(w) for w in weights], after)


def join_kernel(own, r1, r2, r3, *refs):
    out = refs[-1]
    out[...] = jnp.concatenate([ref[...].astype(F32) for ref in (own, r1, r2, r3)], axis=0).astype(
        out.dtype
    )


def stack_kernel(a_ref, b_ref, unread, out):
    rows = a_ref.shape[0]
    out[:rows, :] = a_ref[...]
    out[rows:, :] = b_ref[...]


def expert_kernel(scale, *refs):
    blocks = refs[:16]
    gate_ref, up_ref, down_ref = refs[16:19]
    outs = refs[19:35]
    balance_ref, hidden_ref, x_ref = refs[35:]
    width = down_ref.shape[1]
    rows = blocks[0].shape[0]
    tile = 512

    for n, block in enumerate(blocks):
        x_ref[n * rows : (n + 1) * rows, :] = block[:, :width]
    gate = jnp.dot(x_ref[...], gate_ref[...], preferred_element_type=F32)
    up = jnp.dot(x_ref[...], up_ref[...], preferred_element_type=F32)
    hidden_ref[...] = (gate * jax.nn.sigmoid(gate) * up).astype(BF16)

    def down(i, carry):
        at = pl.ds(pl.multiple_of(i * tile, tile), tile)
        value = jnp.dot(hidden_ref[...], down_ref[:, at], preferred_element_type=F32)
        for n, out in enumerate(outs):
            out[:, at] = value[n * rows : (n + 1) * rows, :].astype(out.dtype)
        return carry

    lax.fori_loop(0, width // tile, down, 0)

    total = jnp.zeros((rows, LANES), F32)
    for block in blocks:
        total = total + block[:, width:].astype(F32)
    parity = lax.broadcasted_iota(jnp.int32, total.shape, 0) % 2
    named = jnp.sum(jnp.where(parity == 0, total, 0.0), axis=0, keepdims=True)
    probs = jnp.sum(jnp.where(parity == 1, total, 0.0), axis=0, keepdims=True)
    balance_ref[...] = jnp.sum(named * probs, axis=1, keepdims=True) * scale


def add_kernel(*refs):
    value = refs[0][...]
    for ref in refs[1:-1]:
        value = value + ref[...].astype(F32)
    refs[-1][...] = value.astype(refs[-1].dtype)


def split_kernel(keep_ref, came_ref, a_ref, b_ref):
    rows = a_ref.shape[0]
    total = keep_ref[...] + came_ref[...].astype(F32)
    a_ref[...] = total[:rows]
    b_ref[...] = total[rows:].astype(BF16)


def part_kernel(a_ref, came_ref, own, s1, s2, s3):
    total = a_ref[...] + came_ref[...].astype(F32)
    for j, out in enumerate((own, s1, s2, s3)):
        out[...] = total[j * CAP : (j + 1) * CAP].astype(out.dtype)


def mix_kernel(cw_ref, own, r1, r2, r3, out):
    weights = cw_ref[...]
    total = None
    for j, ref in enumerate((own, r1, r2, r3)):
        value = ref[...].astype(F32)
        for s in range(CAP):
            at = j * CAP + s
            term = weights[:, at : at + 1] * value[s : s + 1, :]
            total = term if total is None else total + term
    out[...] = total.astype(out.dtype)


def to_expert(value, step):
    return lax.ppermute(value, "xo", [(i, (i + step) % EXPERTS) for i in range(EXPERTS)])


def swap(value, axis):
    return lax.ppermute(value, axis, [(0, 1), (1, 0)])


def ring(value, back):
    pairs = []
    for y in range(RING):
        for c in range(CORES):
            step = 1 if (c == 0) != back else -1
            pairs.append((y * CORES + c, (y + step) % RING * CORES + c))
    return lax.ppermute(value, ("y", "core"), pairs)


def local(tokens, router_weight, expert_ids, slots, gate_weight, up_weight, down_weight):
    devices = lax.axis_size(EXPERT)
    count, width = tokens.shape
    wide = width + LANES
    hbm = pl.BlockSpec(memory_space=pltpu.HBM)
    anyway = pl.BlockSpec(memory_space=pl.ANY)
    *sends, weights = call(
        pack_kernel,
        [shape(CAP, wide, BF16)] * EXPERTS + [shape(count, LANES, F32)],
        [in_hbm(a) for a in (expert_ids.T, slots.T, tokens, router_weight.T)],
        in_specs=[hbm] * 4,
        scratch=[
            pltpu.VMEM(tokens.shape, BF16),
            pltpu.VMEM(router_weight.shape[::-1], BF16),
            pltpu.SMEM(slots.shape[::-1], jnp.int32),
            pltpu.SMEM(slots.shape[::-1], jnp.int32),
            pltpu.SemaphoreType.DMA((4,)),
        ],
    )
    arrived = [sends[0]] + [to_expert(sends[k], k) for k in range(1, EXPERTS)]
    down_near = fetch([down_weight], sends[0])
    size = EXPERTS * CAP
    block = call(
        join_kernel,
        [shape(size, wide, BF16)],
        (*arrived, down_near[0]),
        in_specs=vmem(EXPERTS) + [anyway],
    )[0]
    gate_near = fetch([gate_weight, up_weight], block)
    mine = call(
        stack_kernel,
        [shape(2 * size, wide, BF16)],
        (block, swap(block, "xi"), gate_near[0]),
        in_specs=vmem(2) + [anyway],
    )[0]
    theirs = swap(mine, "core")

    got = {}
    for chunk, start in ((0, mine), (1, theirs)):
        moving = start
        for d in range(1, HALF + 1 - chunk):
            moving = ring(moving, False)
            got[chunk, d] = moving
    near = [got[key] for key in BLOCKS]
    far = [swap(block, "core") for block in near]

    rows = 2 * size
    total_tokens = count * devices
    scale = EXPERTS / (2.0 * total_tokens * total_tokens)
    outs = pl.pallas_call(
        lambda *refs: expert_kernel(scale, *refs),
        out_shape=[shape(rows, width, F32)] * 9
        + [shape(rows, width, BF16)] * 7
        + [shape(1, 1, F32)],
        in_specs=vmem(19),
        out_specs=vmem(17),
        scratch_shapes=[
            pltpu.VMEM((16 * rows, gate_weight.shape[1]), BF16),
            pltpu.VMEM((16 * rows, width), BF16),
        ],
        cost_estimate=pl.CostEstimate(
            flops=6 * 16 * rows * width * gate_weight.shape[1],
            bytes_accessed=18_000_000,
            transcendentals=0,
        ),
        compiler_params=pltpu.CompilerParams(vmem_limit_bytes=28 << 20),
    )(mine, theirs, *near, *far, *gate_near, *down_near)
    own_mine, own_theirs = outs[:2]
    kept = dict(zip(BLOCKS, outs[2:9]))
    crossed = {key: swap(value, "core") for key, value in reversed(list(zip(BLOCKS, outs[9:16])))}
    balance = outs[16].reshape(1)

    moving = {}
    for d in range(HALF, 0, -1):
        for chunk in (0, 1):
            if (chunk, d) in kept:
                terms = [kept[chunk, d], crossed[chunk, d]]
                if chunk in moving:
                    terms.append(moving[chunk])
                value = call(add_kernel, [shape(rows, width, BF16)], terms)[0]
                moving[chunk] = ring(value, True)
    cross = call(add_kernel, [shape(rows, width, BF16)], (own_theirs, moving[1]))[0]
    came = swap(cross, "core")
    keep = call(add_kernel, [shape(rows, width, F32)], (own_mine, moving[0]))[0]
    a_sum, b_sum = call(
        split_kernel, [shape(size, width, F32), shape(size, width, BF16)], (keep, came)
    )
    pieces = call(
        part_kernel,
        [shape(CAP, width, F32)] + [shape(CAP, width, BF16)] * 3,
        (a_sum, swap(b_sum, "xi")),
    )
    returned = [pieces[0]] + [to_expert(pieces[k], -k) for k in range(1, EXPERTS)]
    mixed_rows = call(mix_kernel, [shape(count, width, BF16)], (weights, *returned))[0]
    return (mixed_rows, balance)


def solution(mesh):
    split = Mesh(
        mesh.devices.reshape(mesh.shape["groups"], EXPERTS, PAIR, RING, CORES),
        GROUPS_EXPERT,
    )
    placed = (
        P(GROUPS_EXPERT, None),
        P("groups", None),
        P(GROUPS_EXPERT, None),
        P(GROUPS_EXPERT, None),
        P(None, EXPERT),
        P(None, EXPERT),
        P(EXPERT, None),
    )
    return jax.shard_map(
        local,
        mesh=split,
        in_specs=placed,
        out_specs=(P(GROUPS_EXPERT, None), P("groups")),
        check_vma=False,
    )
```

```python
import functools

import jax
import jax.numpy as jnp
from jax import lax
from jax.experimental import pallas as pl
from jax.experimental.pallas import tpu as pltpu
from jax.sharding import Mesh
from jax.sharding import PartitionSpec as P

EXPERTS = 4
CAP = 2
PAIR, RING, CORES = 2, 8, 2
LANES = 128
EXPERT = ("xo", "xi", "y", "core")
GROUPS_EXPERT = ("groups",) + EXPERT
F32, BF16 = jnp.float32, jnp.bfloat16
HALF = RING // 2
REACH = {(0, 1): HALF, (0, -1): HALF - 1, (1, 1): HALF - 1, (1, -1): HALF}
GROUPS = [
    [(b, sign, d) for d in distances for b in (0, 1) for sign in (1, -1) if d <= REACH[b, sign]]
    for distances in ((1, 2), (3,), (4,))
]


def vmem(count):
    return [pl.BlockSpec(memory_space=pltpu.VMEM)] * count


def call(kernel, outs, args, flops=200_000, in_specs=None, scratch=()):
    size = 1_000_000
    return pl.pallas_call(
        kernel,
        out_shape=outs,
        in_specs=in_specs or vmem(len(args)),
        out_specs=vmem(len(outs)),
        scratch_shapes=list(scratch),
        cost_estimate=pl.CostEstimate(flops=flops, bytes_accessed=size, transcendentals=0),
        compiler_params=pltpu.CompilerParams(vmem_limit_bytes=4 << 20),
    )(*args)


def shape(rows, width, dtype):
    return jax.ShapeDtypeStruct((rows, width), dtype)


def column_of(scalars, count):
    row = lax.broadcasted_iota(jnp.int32, (count, 1), 0)
    value = jnp.zeros((count, 1), jnp.int32)
    for t, scalar in enumerate(scalars):
        value = jnp.where(row == t, scalar, value)
    return value


def pack_kernel(
    ids_hbm,
    slots_hbm,
    tok_hbm,
    router_hbm,
    own,
    s1,
    s2,
    s3,
    cw_ref,
    tok_ref,
    router_ref,
    ids_s,
    slots_s,
    sems,
):
    copies = [
        pltpu.make_async_copy(tok_hbm, tok_ref, sems.at[0]),
        pltpu.make_async_copy(router_hbm, router_ref, sems.at[1]),
        pltpu.make_async_copy(ids_hbm, ids_s, sems.at[2]),
        pltpu.make_async_copy(slots_hbm, slots_s, sems.at[3]),
    ]
    for copy in copies:
        copy.start()
    here = lax.axis_index("xo")
    count, width = tok_ref.shape
    for copy in copies:
        copy.wait()
    ids = [column_of([ids_s[k, t] for t in range(count)], count) for k in range(2)]
    slots = [column_of([slots_s[k, t] for t in range(count)], count) for k in range(2)]
    tok = tok_ref[...].astype(F32)
    router = router_ref[...].astype(F32)
    logits = [
        jnp.sum(tok * router[e : e + 1, :], axis=1, keepdims=True) for e in range(EXPERTS)
    ]
    top = jnp.maximum(jnp.maximum(logits[0], logits[1]), jnp.maximum(logits[2], logits[3]))
    raised = [jnp.exp(v - top) for v in logits]
    inverse = 1.0 / (raised[0] + raised[1] + raised[2] + raised[3])
    lane = lax.broadcasted_iota(jnp.int32, (1, LANES), 1)
    count_row = jnp.zeros((1, LANES), F32)
    prob_row = jnp.zeros((1, LANES), F32)
    for e in range(EXPERTS):
        named = jnp.sum(
            (ids[0] == e).astype(F32) + (ids[1] == e).astype(F32), axis=0, keepdims=True
        )
        prob = jnp.sum(raised[e] * inverse, axis=0, keepdims=True)
        high = prob.astype(BF16).astype(F32)
        count_row = jnp.where((lane == e) | (lane == e + EXPERTS), named, count_row)
        prob_row = jnp.where(lane == e, high, prob_row)
        prob_row = jnp.where(lane == e + EXPERTS, prob - high, prob_row)
    statistic = jnp.concatenate([count_row, prob_row], axis=0).astype(BF16)
    chosen = []
    for k in range(2):
        picked = jnp.zeros_like(logits[0])
        for e in range(EXPERTS):
            picked = jnp.where(ids[k] == e, logits[e], picked)
        chosen.append(picked)
    top = jnp.maximum(chosen[0], chosen[1])
    chosen = [jnp.exp(v - top) for v in chosen]
    total = chosen[0] + chosen[1]
    gates = [v / total for v in chosen]
    lane = lax.broadcasted_iota(jnp.int32, (count, LANES), 1)
    weights = jnp.zeros((count, LANES), F32)
    for j, out in enumerate((own, s1, s2, s3)):
        expert = lax.rem(here + j, EXPERTS)
        rows = []
        for s in range(CAP):
            row = jnp.zeros((1, width), F32)
            for t in range(count):
                hit = ((ids_s[0, t] == expert) & (slots_s[0, t] == s)) | (
                    (ids_s[1, t] == expert) & (slots_s[1, t] == s)
                )
                row = jnp.where(hit, tok[t : t + 1, :], row)
            rows.append(row)
            column = jnp.zeros((count, 1), F32)
            for k in range(2):
                match = (ids[k] == expert) & (slots[k] == s)
                column = jnp.where(match, gates[k], column)
            weights = jnp.where(lane == j * CAP + s, column, weights)
        out[:, :width] = jnp.concatenate(rows, axis=0).astype(BF16)
        out[:, width:] = statistic
    cw_ref[...] = weights


def in_hbm(value):
    return pltpu.with_memory_space_constraint(value, pltpu.HBM)


def join_kernel(own, r1, r2, r3, out):
    out[...] = jnp.concatenate([ref[...].astype(F32) for ref in (own, r1, r2, r3)], axis=0).astype(
        out.dtype
    )


def stack_kernel(count, *refs):
    start = 0
    for ref in refs[:count]:
        refs[-1][start : start + ref.shape[0], :] = ref[...]
        start += ref.shape[0]


def expert_kernel(scale, *refs):
    blocks, (gate_hbm, up_hbm, down_hbm) = refs[:6], refs[6:9]
    outs, balance_ref = refs[9:15], refs[15]
    x_ref, hidden_ref, gate_ref, up_ref, down_ref, sems = refs[16:]
    width = down_ref.shape[1]
    cuts = 4
    depth = width // cuts
    copies = []
    for n in range(cuts):
        at = pl.ds(n * depth, depth)
        copies.append(pltpu.make_async_copy(gate_hbm.at[at], gate_ref.at[at], sems.at[2 * n]))
        copies.append(pltpu.make_async_copy(up_hbm.at[at], up_ref.at[at], sems.at[2 * n + 1]))
    copies.append(pltpu.make_async_copy(down_hbm, down_ref, sems.at[2 * cuts]))
    for copy in copies:
        copy.start()
    start = 0
    total = jnp.zeros((8, LANES), F32)
    for block in blocks:
        rows = block.shape[0]
        x_ref[start : start + rows, :] = block[:, :width]
        start += rows
        for n in range(0, rows, 8):
            total = total + block[n : n + 8, width:].astype(F32)
    parity = lax.broadcasted_iota(jnp.int32, total.shape, 0) % 2
    named = jnp.sum(jnp.where(parity == 0, total, 0.0), axis=0, keepdims=True)
    probs = jnp.sum(jnp.where(parity == 1, total, 0.0), axis=0, keepdims=True)
    balance_ref[...] = jnp.sum(named * probs, axis=1, keepdims=True) * scale

    gate = up = None
    for n in range(cuts):
        copies[2 * n].wait()
        copies[2 * n + 1].wait()
        at = slice(n * depth, (n + 1) * depth)
        x = x_ref[:, at]
        g = jnp.dot(x, gate_ref[at, :], preferred_element_type=F32)
        u = jnp.dot(x, up_ref[at, :], preferred_element_type=F32)
        gate, up = (g, u) if n == 0 else (gate + g, up + u)
    hidden_ref[...] = (gate * jax.nn.sigmoid(gate) * up).astype(BF16)
    copies[2 * cuts].wait()
    tile = 512

    def down(i, carry):
        at = pl.ds(pl.multiple_of(i * tile, tile), tile)
        value = jnp.dot(hidden_ref[...], down_ref[:, at], preferred_element_type=F32)
        start = 0
        for out in outs:
            out[:, at] = value[start : start + out.shape[0], :].astype(out.dtype)
            start += out.shape[0]
        return carry

    lax.fori_loop(0, width // tile, down, 0)


def add_kernel(start, kept_ref, crossed_ref, *refs):
    out = refs[-1]
    at = slice(start, start + out.shape[0])
    value = kept_ref[at, :] + crossed_ref[at, :].astype(F32)
    for ref in refs[:-1]:
        value = value + ref[...].astype(F32)
    out[...] = value.astype(out.dtype)


def part_kernel(a_ref, came_ref, own, s1, s2, s3):
    total = a_ref[...] + came_ref[...].astype(F32)
    for j, out in enumerate((own, s1, s2, s3)):
        out[...] = total[j * CAP : (j + 1) * CAP].astype(out.dtype)


def mix_kernel(cw_ref, own, r1, r2, r3, out):
    weights = cw_ref[...]
    total = None
    for j, ref in enumerate((own, r1, r2, r3)):
        value = ref[...].astype(F32)
        for s in range(CAP):
            at = j * CAP + s
            term = weights[:, at : at + 1] * value[s : s + 1, :]
            total = term if total is None else total + term
    out[...] = total.astype(out.dtype)


def in_hbm(value):
    return pltpu.with_memory_space_constraint(value, pltpu.HBM)


def to_expert(value, step):
    return lax.ppermute(value, "xo", [(i, (i + step) % EXPERTS) for i in range(EXPERTS)])


def swap(value, axis):
    return lax.ppermute(value, axis, [(0, 1), (1, 0)])


def along(value, step):
    return lax.ppermute(value, "y", [(y, (y + step) % RING) for y in range(RING)])


def local(tokens, router_weight, expert_ids, slots, gate_weight, up_weight, down_weight):
    devices = lax.axis_size(EXPERT)
    count, width = tokens.shape
    wide = width + LANES
    hbm = pl.BlockSpec(memory_space=pltpu.HBM)
    *sends, weights = call(
        pack_kernel,
        [shape(CAP, wide, BF16)] * EXPERTS + [shape(count, LANES, F32)],
        [in_hbm(a) for a in (expert_ids.T, slots.T, tokens, router_weight.T)],
        in_specs=[hbm] * 4,
        scratch=[
            pltpu.VMEM(tokens.shape, BF16),
            pltpu.VMEM(router_weight.shape[::-1], BF16),
            pltpu.SMEM(slots.shape[::-1], jnp.int32),
            pltpu.SMEM(slots.shape[::-1], jnp.int32),
            pltpu.SemaphoreType.DMA((4,)),
        ],
    )
    arrived = [sends[0]] + [to_expert(sends[k], k) for k in range(1, EXPERTS)]
    size = EXPERTS * CAP
    block_a = call(join_kernel, [shape(size, wide, BF16)], arrived)[0]
    block_b = swap(block_a, "xi")

    got = {}
    for b, block in enumerate((block_a, block_b)):
        for sign in (1, -1):
            moving = block
            for d in range(1, REACH[b, sign] + 1):
                moving = along(moving, sign)
                got[b, sign, d] = moving
    parts = [[got[key] for key in keys] for keys in GROUPS]
    parts[0] = [block_a, block_b] + parts[0]
    rows = [size * len(part) for part in parts]
    near = []
    for group, part in enumerate(parts):
        behind = parts[1] if group == 0 else []
        near += call(
            functools.partial(stack_kernel, len(part)),
            [shape(rows[group], wide, BF16)],
            part + behind,
            in_specs=vmem(len(part)) + [pl.BlockSpec(memory_space=pl.ANY)] * len(behind),
        )
    far = [swap(group, "core") for group in near]

    units = gate_weight.shape[1]
    total_tokens = count * devices
    scale = EXPERTS / (2.0 * total_tokens * total_tokens)
    outs = pl.pallas_call(
        lambda *refs: expert_kernel(scale, *refs),
        out_shape=[shape(n, width, F32) for n in rows]
        + [shape(n, width, BF16) for n in rows]
        + [shape(1, 1, F32)],
        in_specs=vmem(6) + [hbm] * 3,
        out_specs=vmem(7),
        scratch_shapes=[
            pltpu.VMEM((2 * sum(rows), width), BF16),
            pltpu.VMEM((2 * sum(rows), units), BF16),
            pltpu.VMEM((width, units), BF16),
            pltpu.VMEM((width, units), BF16),
            pltpu.VMEM((units, width), BF16),
            pltpu.SemaphoreType.DMA((9,)),
        ],
        cost_estimate=pl.CostEstimate(
            flops=12 * sum(rows) * width * units, bytes_accessed=18_000_000, transcendentals=0
        ),
        compiler_params=pltpu.CompilerParams(vmem_limit_bytes=28 << 20),
    )(*near, *far, *[in_hbm(w) for w in (gate_weight, up_weight, down_weight)])
    kept = outs[:3]
    crossed = [swap(value, "core") for value in reversed(outs[3:6])][::-1]
    balance = outs[6].reshape(1)

    moving = {}
    for group in reversed(range(len(GROUPS))):
        for d in sorted({key[2] for key in GROUPS[group]}, reverse=True):
            for b, sign in REACH:
                key = (b, sign, d)
                if key not in GROUPS[group]:
                    continue
                start = size * (GROUPS[group].index(key) + (2 if group == 0 else 0))
                came = [moving[b, sign]] if (b, sign) in moving else []
                value = call(
                    functools.partial(add_kernel, start),
                    [shape(size, width, BF16)],
                    [kept[group], crossed[group]] + came,
                )[0]
                moving[b, sign] = along(value, -sign)
    sums = []
    for b, dtype in ((1, BF16), (0, F32)):
        sums += call(
            functools.partial(add_kernel, b * size),
            [shape(size, width, dtype)],
            (kept[0], crossed[0], moving[b, 1], moving[b, -1]),
        )
    pieces = call(
        part_kernel,
        [shape(CAP, width, F32)] + [shape(CAP, width, BF16)] * 3,
        (sums[1], swap(sums[0], "xi")),
    )
    returned = [pieces[0]] + [to_expert(pieces[k], -k) for k in range(1, EXPERTS)]
    mixed_rows = call(mix_kernel, [shape(count, width, BF16)], (weights, *returned))[0]
    return (mixed_rows, balance)


def solution(mesh):
    split = Mesh(
        mesh.devices.reshape(mesh.shape["groups"], EXPERTS, PAIR, RING, CORES),
        GROUPS_EXPERT,
    )
    placed = (
        P(GROUPS_EXPERT, None),
        P("groups", None),
        P(GROUPS_EXPERT, None),
        P(GROUPS_EXPERT, None),
        P(None, EXPERT),
        P(None, EXPERT),
        P(EXPERT, None),
    )
    return jax.shard_map(
        local,
        mesh=split,
        in_specs=placed,
        out_specs=(P(GROUPS_EXPERT, None), P("groups")),
        check_vma=False,
    )
```

```python
import functools

import jax
import jax.numpy as jnp
from jax import lax
from jax.experimental import pallas as pl
from jax.experimental.pallas import tpu as pltpu
from jax.sharding import Mesh
from jax.sharding import PartitionSpec as P


EXPERTS = 4
CAP = 2
PAIR, RING, CORES = 2, 8, 2
LANES = 128
CUTS = 1
STEP = 64
EXPERT = ("xo", "xi", "y", "core")
GROUPS_EXPERT = ("groups",) + EXPERT
F32, BF16 = jnp.float32, jnp.bfloat16
HALF = RING // 2
REACH = {(0, 1): HALF, (0, -1): HALF - 1, (1, 1): HALF - 1, (1, -1): HALF}
GROUPS = [
    [(b, sign, d) for d in distances for b in (0, 1) for sign in (1, -1) if d <= REACH[b, sign]]
    for distances in ((1, 2), (3,), (4,))
]


def vmem(count):
    return [pl.BlockSpec(memory_space=pltpu.VMEM)] * count


def call(kernel, outs, args, flops=200_000, in_specs=None, scratch=()):
    size = 1_000_000
    return pl.pallas_call(
        kernel,
        out_shape=outs,
        in_specs=in_specs or vmem(len(args)),
        out_specs=vmem(len(outs)),
        scratch_shapes=list(scratch),
        cost_estimate=pl.CostEstimate(flops=flops, bytes_accessed=size, transcendentals=0),
        compiler_params=pltpu.CompilerParams(vmem_limit_bytes=4 << 20),
    )(*args)


def shape(rows, width, dtype):
    return jax.ShapeDtypeStruct((rows, width), dtype)


def column_of(scalars, count):
    row = lax.broadcasted_iota(jnp.int32, (count, 1), 0)
    value = jnp.zeros((count, 1), jnp.int32)
    for t, scalar in enumerate(scalars):
        value = jnp.where(row == t, scalar, value)
    return value


def pack_kernel(
    ids_hbm,
    slots_hbm,
    tok_hbm,
    router_hbm,
    own,
    s1,
    s2,
    s3,
    cw_ref,
    tok_ref,
    router_ref,
    ids_s,
    slots_s,
    sems,
):
    copies = [
        pltpu.make_async_copy(tok_hbm, tok_ref, sems.at[0]),
        pltpu.make_async_copy(router_hbm, router_ref, sems.at[1]),
        pltpu.make_async_copy(ids_hbm, ids_s, sems.at[2]),
        pltpu.make_async_copy(slots_hbm, slots_s, sems.at[3]),
    ]
    for copy in copies:
        copy.start()
    here = lax.axis_index("xo")
    count, width = tok_ref.shape
    for copy in copies:
        copy.wait()
    ids = [column_of([ids_s[k, t] for t in range(count)], count) for k in range(2)]
    slots = [column_of([slots_s[k, t] for t in range(count)], count) for k in range(2)]
    tok = tok_ref[...].astype(F32)
    router = router_ref[...].astype(F32)
    logits = [
        jnp.sum(tok * router[e : e + 1, :], axis=1, keepdims=True) for e in range(EXPERTS)
    ]
    top = jnp.maximum(jnp.maximum(logits[0], logits[1]), jnp.maximum(logits[2], logits[3]))
    raised = [jnp.exp(v - top) for v in logits]
    inverse = 1.0 / (raised[0] + raised[1] + raised[2] + raised[3])
    lane = lax.broadcasted_iota(jnp.int32, (1, LANES), 1)
    count_row = jnp.zeros((1, LANES), F32)
    prob_row = jnp.zeros((1, LANES), F32)
    for e in range(EXPERTS):
        named = jnp.sum(
            (ids[0] == e).astype(F32) + (ids[1] == e).astype(F32), axis=0, keepdims=True
        )
        prob = jnp.sum(raised[e] * inverse, axis=0, keepdims=True)
        high = prob.astype(BF16).astype(F32)
        count_row = jnp.where((lane == e) | (lane == e + EXPERTS), named, count_row)
        prob_row = jnp.where(lane == e, high, prob_row)
        prob_row = jnp.where(lane == e + EXPERTS, prob - high, prob_row)
    statistic = jnp.concatenate([count_row, prob_row], axis=0).astype(BF16)
    chosen = []
    for k in range(2):
        picked = jnp.zeros_like(logits[0])
        for e in range(EXPERTS):
            picked = jnp.where(ids[k] == e, logits[e], picked)
        chosen.append(picked)
    top = jnp.maximum(chosen[0], chosen[1])
    chosen = [jnp.exp(v - top) for v in chosen]
    total = chosen[0] + chosen[1]
    gates = [v / total for v in chosen]
    lane = lax.broadcasted_iota(jnp.int32, (count, LANES), 1)
    weights = jnp.zeros((count, LANES), F32)
    for j, out in enumerate((own, s1, s2, s3)):
        expert = lax.rem(here + j, EXPERTS)
        rows = []
        for s in range(CAP):
            row = jnp.zeros((1, width), F32)
            for t in range(count):
                hit = ((ids_s[0, t] == expert) & (slots_s[0, t] == s)) | (
                    (ids_s[1, t] == expert) & (slots_s[1, t] == s)
                )
                row = jnp.where(hit, tok[t : t + 1, :], row)
            rows.append(row)
            column = jnp.zeros((count, 1), F32)
            for k in range(2):
                match = (ids[k] == expert) & (slots[k] == s)
                column = jnp.where(match, gates[k], column)
            weights = jnp.where(lane == j * CAP + s, column, weights)
        out[:, :width] = jnp.concatenate(rows, axis=0).astype(BF16)
        out[:, width:] = statistic
    cw_ref[...] = weights


def in_hbm(value):
    return pltpu.with_memory_space_constraint(value, pltpu.HBM)


def join_kernel(own, r1, r2, r3, unread, out):
    out[...] = jnp.concatenate([ref[...].astype(F32) for ref in (own, r1, r2, r3)], axis=0).astype(
        out.dtype
    )


def stack_kernel(count, *refs):
    start = 0
    for ref in refs[:count]:
        refs[-1][start : start + ref.shape[0], :] = ref[...]
        start += ref.shape[0]


def deep_dot(x_ref, weight_ref, cuts=CUTS):
    depth = weight_ref.shape[0] // cuts
    total = None
    for n in range(cuts):
        at = slice(n * depth, (n + 1) * depth)
        value = jnp.dot(x_ref[:, at], weight_ref[at, :], preferred_element_type=F32)
        total = value if n == 0 else total + value
    return total


def expert_rows(near, far, x_ref, hidden_ref, gate_ref, up_ref, down_ref, outs, lanes, ready):
    width = down_ref.shape[1]
    start = 0
    total = jnp.zeros((8, LANES), F32)
    for block in near + far:
        rows = block.shape[0]
        x_ref[start : start + rows, :] = block[:, :width]
        start += rows
        for n in range(0, rows, 8):
            total = total + block[n : n + 8, width:].astype(F32)
    lanes(total)
    gate = deep_dot(x_ref, gate_ref)
    ready()
    up = deep_dot(x_ref, up_ref)
    hidden_ref[...] = (gate * jax.nn.sigmoid(gate) * up).astype(BF16)
    tile = 512

    def down(i, carry):
        at = pl.ds(pl.multiple_of(i * tile, tile), tile)
        value = jnp.dot(hidden_ref[...], down_ref[:, at], preferred_element_type=F32)
        start = 0
        for out in outs:
            out[:, at] = value[start : start + out.shape[0], :].astype(out.dtype)
            start += out.shape[0]
        return carry

    lax.fori_loop(0, width // tile, down, 0)


def first_kernel(near, far, gate, down, up_hbm, kept, sent, up_ref, total_ref, x, hidden, sem):
    copy = pltpu.make_async_copy(up_hbm, up_ref, sem.at[0])
    copy.start()

    def lanes(total):
        total_ref[...] = total

    expert_rows([near], [far], x, hidden, gate, up_ref, down, [kept, sent], lanes, copy.wait)


def second_kernel(scale, near, near_4, far, far_4, gate, up, down, before, *refs):
    outs, balance_ref, x, hidden = refs[:4], refs[4], refs[5], refs[6]

    def lanes(total):
        total = before[...] + total
        parity = lax.broadcasted_iota(jnp.int32, total.shape, 0) % 2
        named = jnp.sum(jnp.where(parity == 0, total, 0.0), axis=0, keepdims=True)
        probs = jnp.sum(jnp.where(parity == 1, total, 0.0), axis=0, keepdims=True)
        balance_ref[...] = jnp.sum(named * probs, axis=1, keepdims=True) * scale

    expert_rows(
        [near, near_4], [far, far_4], x, hidden, gate, up, down, outs, lanes, lambda: None
    )


def fetch_kernel(*refs):
    count = (len(refs) - 2) // 2
    copies = [
        pltpu.make_async_copy(refs[n], refs[count + 1 + n], refs[-1].at[n]) for n in range(count)
    ]
    for copy in copies:
        copy.start()
    for copy in copies:
        copy.wait()


def fetch(weights, after):
    return pl.pallas_call(
        fetch_kernel,
        out_shape=[pltpu.VMEM(w.shape, w.dtype) for w in weights],
        in_specs=[pl.BlockSpec(memory_space=pltpu.HBM)] * len(weights)
        + [pl.BlockSpec(memory_space=pl.ANY)],
        out_specs=vmem(len(weights)),
        scratch_shapes=[pltpu.SemaphoreType.DMA((len(weights),))],
        cost_estimate=pl.CostEstimate(
            flops=1_000_000,
            bytes_accessed=sum(2 * w.size * w.dtype.itemsize for w in weights),
            transcendentals=0,
        ),
        compiler_params=pltpu.CompilerParams(vmem_limit_bytes=4 << 20),
    )(*[in_hbm(w) for w in weights], after)


def add_kernel(start, kept_ref, crossed_ref, *refs):
    out = refs[-1]
    at = slice(start, start + out.shape[0])
    value = kept_ref[at, :] + crossed_ref[at, :].astype(F32)
    for ref in refs[:-1]:
        value = value + ref[...].astype(F32)
    out[...] = value.astype(out.dtype)


def part_kernel(a_ref, came_ref, own, s1, s2, s3):
    total = a_ref[...] + came_ref[...].astype(F32)
    for j, out in enumerate((own, s1, s2, s3)):
        out[...] = total[j * CAP : (j + 1) * CAP].astype(out.dtype)


def mix_kernel(cw_ref, own, r1, r2, r3, out):
    weights = cw_ref[...]
    total = None
    for j, ref in enumerate((own, r1, r2, r3)):
        value = ref[...].astype(F32)
        for s in range(CAP):
            at = j * CAP + s
            term = weights[:, at : at + 1] * value[s : s + 1, :]
            total = term if total is None else total + term
    out[...] = total.astype(out.dtype)


def in_hbm(value):
    return pltpu.with_memory_space_constraint(value, pltpu.HBM)


def to_expert(value, step):
    return lax.ppermute(value, "xo", [(i, (i + step) % EXPERTS) for i in range(EXPERTS)])


def swap(value, axis):
    return lax.ppermute(value, axis, [(0, 1), (1, 0)])


def along(value, step):
    return lax.ppermute(value, "y", [(y, (y + step) % RING) for y in range(RING)])


def local(tokens, router_weight, expert_ids, slots, gate_weight, up_weight, down_weight):
    devices = lax.axis_size(EXPERT)
    count, width = tokens.shape
    wide = width + LANES
    hbm = pl.BlockSpec(memory_space=pltpu.HBM)
    *sends, weights = call(
        pack_kernel,
        [shape(CAP, wide, BF16)] * EXPERTS + [shape(count, LANES, F32)],
        [in_hbm(a) for a in (expert_ids.T, slots.T, tokens, router_weight.T)],
        in_specs=[hbm] * 4,
        scratch=[
            pltpu.VMEM(tokens.shape, BF16),
            pltpu.VMEM(router_weight.shape[::-1], BF16),
            pltpu.SMEM(slots.shape[::-1], jnp.int32),
            pltpu.SMEM(slots.shape[::-1], jnp.int32),
            pltpu.SemaphoreType.DMA((4,)),
        ],
    )
    arrived = [sends[0]] + [to_expert(sends[k], k) for k in range(1, EXPERTS)]
    size = EXPERTS * CAP
    gate_near, down_near = fetch([gate_weight, down_weight], sends[0])
    block_a = call(
        join_kernel,
        [shape(size, wide, BF16)],
        (*arrived, gate_near),
        in_specs=vmem(EXPERTS) + [pl.BlockSpec(memory_space=pl.ANY)],
    )[0]
    block_b = swap(block_a, "xi")

    got = {}
    for b, block in enumerate((block_a, block_b)):
        for sign in (1, -1):
            moving = block
            for d in range(1, REACH[b, sign] + 1):
                moving = along(moving, sign)
                got[b, sign, d] = moving
    parts = [[got[key] for key in keys] for keys in GROUPS]
    parts[0] = [block_a, block_b] + parts[0]
    rows = [size * len(part) for part in parts]
    near, far = [], []
    for group, part in enumerate(parts):
        near += call(
            functools.partial(stack_kernel, len(part)), [shape(rows[group], wide, BF16)], part
        )
        far.append(swap(near[group], "core"))

    units = gate_weight.shape[1]
    total_tokens = count * devices
    scale = EXPERTS / (2.0 * total_tokens * total_tokens)

    def expert(kernel, rows, args, in_specs, outs, scratch=()):
        return pl.pallas_call(
            kernel,
            out_shape=[shape(n, width, dtype) for dtype in (F32, BF16) for n in rows] + outs,
            in_specs=in_specs,
            out_specs=vmem(2 * len(rows) + len(outs)),
            scratch_shapes=[
                pltpu.VMEM((-(-2 * sum(rows) // STEP) * STEP, width), BF16),
                pltpu.VMEM((-(-2 * sum(rows) // STEP) * STEP, units), BF16),
                *scratch,
            ],
            cost_estimate=pl.CostEstimate(
                flops=12 * sum(rows) * width * units, bytes_accessed=9_000_000, transcendentals=0
            ),
            compiler_params=pltpu.CompilerParams(vmem_limit_bytes=24 << 20),
        )(*args)

    *first, up_near, total = expert(
        first_kernel,
        rows[:1],
        (near[0], far[0], gate_near, down_near, in_hbm(up_weight)),
        vmem(4) + [hbm],
        [pltpu.VMEM(up_weight.shape, BF16), shape(8, LANES, F32)],
        [pltpu.SemaphoreType.DMA((1,))],
    )
    *second, balance = expert(
        functools.partial(second_kernel, scale),
        rows[1:],
        (*near[1:], *far[1:], gate_near, up_near, down_near, total),
        vmem(8),
        [shape(1, 1, F32)],
    )
    balance = balance.reshape(1)
    kept = [first[0], second[0], second[1]]
    crossed = {}
    for group, value in ((2, second[3]), (1, second[2]), (0, first[1])):
        crossed[group] = swap(value, "core")

    moving = {}
    for group in reversed(range(len(GROUPS))):
        for d in sorted({key[2] for key in GROUPS[group]}, reverse=True):
            for b, sign in REACH:
                key = (b, sign, d)
                if key not in GROUPS[group]:
                    continue
                start = size * (GROUPS[group].index(key) + (2 if group == 0 else 0))
                came = [moving[b, sign]] if (b, sign) in moving else []
                value = call(
                    functools.partial(add_kernel, start),
                    [shape(size, width, BF16)],
                    [kept[group], crossed[group]] + came,
                )[0]
                moving[b, sign] = along(value, -sign)
    sums = []
    for b, dtype in ((1, BF16), (0, F32)):
        sums += call(
            functools.partial(add_kernel, b * size),
            [shape(size, width, dtype)],
            (kept[0], crossed[0], moving[b, 1], moving[b, -1]),
        )
    pieces = call(
        part_kernel,
        [shape(CAP, width, F32)] + [shape(CAP, width, BF16)] * 3,
        (sums[1], swap(sums[0], "xi")),
    )
    returned = [pieces[0]] + [to_expert(pieces[k], -k) for k in range(1, EXPERTS)]
    mixed_rows = call(mix_kernel, [shape(count, width, BF16)], (weights, *returned))[0]
    return (mixed_rows, balance)


def solution(mesh):
    split = Mesh(
        mesh.devices.reshape(mesh.shape["groups"], EXPERTS, PAIR, RING, CORES),
        GROUPS_EXPERT,
    )
    placed = (
        P(GROUPS_EXPERT, None),
        P("groups", None),
        P(GROUPS_EXPERT, None),
        P(GROUPS_EXPERT, None),
        P(None, EXPERT),
        P(None, EXPERT),
        P(EXPERT, None),
    )

    return jax.shard_map(
        local,
        mesh=split,
        in_specs=placed,
        out_specs=(P(GROUPS_EXPERT, None), P("groups")),
        check_vma=False,
    )
```

```python
import functools

import jax
import jax.numpy as jnp
from jax import lax
from jax.experimental import pallas as pl
from jax.experimental.pallas import tpu as pltpu
from jax.sharding import Mesh
from jax.sharding import PartitionSpec as P


EXPERTS = 4
CAP = 2
PAIR, RING, CORES = 2, 8, 2
LANES = 128
EXPERT = ("xo", "xi", "y", "core")
GROUPS_EXPERT = ("groups",) + EXPERT
F32, BF16 = jnp.float32, jnp.bfloat16
HALF = RING // 2
REACH = {(0, 1): HALF, (0, -1): HALF - 1, (1, 1): HALF - 1, (1, -1): HALF}
GROUPS = [
    [(b, sign, d) for d in distances for b in (0, 1) for sign in (1, -1) if d <= REACH[b, sign]]
    for distances in ((1,), (2,), (3,), (4,))
]


def vmem(count):
    return [pl.BlockSpec(memory_space=pltpu.VMEM)] * count


def call(kernel, outs, args, flops=200_000, in_specs=None, scratch=()):
    size = 1_000_000
    return pl.pallas_call(
        kernel,
        out_shape=outs,
        in_specs=in_specs or vmem(len(args)),
        out_specs=vmem(len(outs)),
        scratch_shapes=list(scratch),
        cost_estimate=pl.CostEstimate(flops=flops, bytes_accessed=size, transcendentals=0),
        compiler_params=pltpu.CompilerParams(vmem_limit_bytes=4 << 20),
    )(*args)


def shape(rows, width, dtype):
    return jax.ShapeDtypeStruct((rows, width), dtype)


def column_of(scalars, count):
    row = lax.broadcasted_iota(jnp.int32, (count, 1), 0)
    value = jnp.zeros((count, 1), jnp.int32)
    for t, scalar in enumerate(scalars):
        value = jnp.where(row == t, scalar, value)
    return value


def pack_kernel(
    ids_hbm,
    slots_hbm,
    tok_hbm,
    router_hbm,
    own,
    s1,
    s2,
    s3,
    cw_ref,
    tok_ref,
    router_ref,
    ids_s,
    slots_s,
    sems,
):
    copies = [
        pltpu.make_async_copy(tok_hbm, tok_ref, sems.at[0]),
        pltpu.make_async_copy(router_hbm, router_ref, sems.at[1]),
        pltpu.make_async_copy(ids_hbm, ids_s, sems.at[2]),
        pltpu.make_async_copy(slots_hbm, slots_s, sems.at[3]),
    ]
    for copy in copies:
        copy.start()
    here = lax.axis_index("xo")
    count, width = tok_ref.shape
    for copy in copies:
        copy.wait()
    ids = [column_of([ids_s[k, t] for t in range(count)], count) for k in range(2)]
    slots = [column_of([slots_s[k, t] for t in range(count)], count) for k in range(2)]
    tok = tok_ref[...].astype(F32)
    router = router_ref[...].astype(F32)
    logits = [
        jnp.sum(tok * router[e : e + 1, :], axis=1, keepdims=True) for e in range(EXPERTS)
    ]
    top = jnp.maximum(jnp.maximum(logits[0], logits[1]), jnp.maximum(logits[2], logits[3]))
    raised = [jnp.exp(v - top) for v in logits]
    inverse = 1.0 / (raised[0] + raised[1] + raised[2] + raised[3])
    lane = lax.broadcasted_iota(jnp.int32, (1, LANES), 1)
    count_row = jnp.zeros((1, LANES), F32)
    prob_row = jnp.zeros((1, LANES), F32)
    for e in range(EXPERTS):
        named = jnp.sum(
            (ids[0] == e).astype(F32) + (ids[1] == e).astype(F32), axis=0, keepdims=True
        )
        prob = jnp.sum(raised[e] * inverse, axis=0, keepdims=True)
        high = prob.astype(BF16).astype(F32)
        count_row = jnp.where((lane == e) | (lane == e + EXPERTS), named, count_row)
        prob_row = jnp.where(lane == e, high, prob_row)
        prob_row = jnp.where(lane == e + EXPERTS, prob - high, prob_row)
    statistic = jnp.concatenate([count_row, prob_row], axis=0).astype(BF16)
    chosen = []
    for k in range(2):
        picked = jnp.zeros_like(logits[0])
        for e in range(EXPERTS):
            picked = jnp.where(ids[k] == e, logits[e], picked)
        chosen.append(picked)
    top = jnp.maximum(chosen[0], chosen[1])
    chosen = [jnp.exp(v - top) for v in chosen]
    total = chosen[0] + chosen[1]
    gates = [v / total for v in chosen]
    lane = lax.broadcasted_iota(jnp.int32, (count, LANES), 1)
    weights = jnp.zeros((count, LANES), F32)
    for j, out in enumerate((own, s1, s2, s3)):
        expert = lax.rem(here + j, EXPERTS)
        rows = []
        for s in range(CAP):
            row = jnp.zeros((1, width), F32)
            for t in range(count):
                hit = ((ids_s[0, t] == expert) & (slots_s[0, t] == s)) | (
                    (ids_s[1, t] == expert) & (slots_s[1, t] == s)
                )
                row = jnp.where(hit, tok[t : t + 1, :], row)
            rows.append(row)
            column = jnp.zeros((count, 1), F32)
            for k in range(2):
                match = (ids[k] == expert) & (slots[k] == s)
                column = jnp.where(match, gates[k], column)
            weights = jnp.where(lane == j * CAP + s, column, weights)
        out[:, :width] = jnp.concatenate(rows, axis=0).astype(BF16)
        out[:, width:] = statistic
    cw_ref[...] = weights


def in_hbm(value):
    return pltpu.with_memory_space_constraint(value, pltpu.HBM)


def join_kernel(own, r1, r2, r3, unread, out):
    out[...] = jnp.concatenate([ref[...].astype(F32) for ref in (own, r1, r2, r3)], axis=0).astype(
        out.dtype
    )


def stack_kernel(count, *refs):
    start = 0
    for ref in refs[:count]:
        refs[-1][start : start + ref.shape[0], :] = ref[...]
        start += ref.shape[0]


def expert_kernel(scale, groups, *refs):
    blocks, (gate, down, up_hbm) = refs[: 2 * groups], refs[2 * groups : 2 * groups + 3]
    refs = refs[2 * groups + 3 :]
    outs, balance_ref = refs[: 2 * groups], refs[2 * groups]
    x_ref, hidden_ref, up, sem = refs[2 * groups + 1 :]
    width = down.shape[1]
    copy = pltpu.make_async_copy(up_hbm, up, sem.at[0])
    copy.start()
    start = 0
    total = jnp.zeros((8, LANES), F32)
    for block in blocks:
        rows = block.shape[0]
        x_ref[start : start + rows, :] = block[:, :width]
        start += rows
        for n in range(0, rows, 8):
            total = total + block[n : n + 8, width:].astype(F32)
    parity = lax.broadcasted_iota(jnp.int32, total.shape, 0) % 2
    named = jnp.sum(jnp.where(parity == 0, total, 0.0), axis=0, keepdims=True)
    probs = jnp.sum(jnp.where(parity == 1, total, 0.0), axis=0, keepdims=True)
    balance_ref[...] = jnp.sum(named * probs, axis=1, keepdims=True) * scale

    gate_pre = jnp.dot(x_ref[...], gate[...], preferred_element_type=F32)
    copy.wait()
    up_pre = jnp.dot(x_ref[...], up[...], preferred_element_type=F32)
    hidden_ref[...] = (gate_pre * jax.nn.sigmoid(gate_pre) * up_pre).astype(BF16)
    tile = 512

    def lower(i, carry):
        at = pl.ds(pl.multiple_of(i * tile, tile), tile)
        value = jnp.dot(hidden_ref[...], down[:, at], preferred_element_type=F32)
        start = 0
        for out in outs:
            out[:, at] = value[start : start + out.shape[0], :].astype(out.dtype)
            start += out.shape[0]
        return carry

    lax.fori_loop(0, width // tile, lower, 0)


def fetch_kernel(*refs):
    count = (len(refs) - 2) // 2
    copies = [
        pltpu.make_async_copy(refs[n], refs[count + 1 + n], refs[-1].at[n]) for n in range(count)
    ]
    for copy in copies:
        copy.start()
    for copy in copies:
        copy.wait()


def fetch(weights, after):
    return pl.pallas_call(
        fetch_kernel,
        out_shape=[pltpu.VMEM(w.shape, w.dtype) for w in weights],
        in_specs=[pl.BlockSpec(memory_space=pltpu.HBM)] * len(weights)
        + [pl.BlockSpec(memory_space=pl.ANY)],
        out_specs=vmem(len(weights)),
        scratch_shapes=[pltpu.SemaphoreType.DMA((len(weights),))],
        cost_estimate=pl.CostEstimate(
            flops=1_000_000,
            bytes_accessed=sum(2 * w.size * w.dtype.itemsize for w in weights),
            transcendentals=0,
        ),
        compiler_params=pltpu.CompilerParams(vmem_limit_bytes=4 << 20),
    )(*[in_hbm(w) for w in weights], after)


def add_kernel(start, kept_ref, crossed_ref, *refs):
    out = refs[-1]
    at = slice(start, start + out.shape[0])
    value = kept_ref[at, :] + crossed_ref[at, :].astype(F32)
    for ref in refs[:-1]:
        value = value + ref[...].astype(F32)
    out[...] = value.astype(out.dtype)


def part_kernel(a_ref, came_ref, own, s1, s2, s3):
    total = a_ref[...] + came_ref[...].astype(F32)
    for j, out in enumerate((own, s1, s2, s3)):
        out[...] = total[j * CAP : (j + 1) * CAP].astype(out.dtype)


def mix_kernel(cw_ref, own, r1, r2, r3, out):
    weights = cw_ref[...]
    total = None
    for j, ref in enumerate((own, r1, r2, r3)):
        value = ref[...].astype(F32)
        for s in range(CAP):
            at = j * CAP + s
            term = weights[:, at : at + 1] * value[s : s + 1, :]
            total = term if total is None else total + term
    out[...] = total.astype(out.dtype)


def in_hbm(value):
    return pltpu.with_memory_space_constraint(value, pltpu.HBM)


def to_expert(value, step):
    return lax.ppermute(value, "xo", [(i, (i + step) % EXPERTS) for i in range(EXPERTS)])


def swap(value, axis):
    return lax.ppermute(value, axis, [(0, 1), (1, 0)])


def along(value, step):
    return lax.ppermute(value, "y", [(y, (y + step) % RING) for y in range(RING)])


def local(tokens, router_weight, expert_ids, slots, gate_weight, up_weight, down_weight):
    devices = lax.axis_size(EXPERT)
    count, width = tokens.shape
    wide = width + LANES
    hbm = pl.BlockSpec(memory_space=pltpu.HBM)
    *sends, weights = call(
        pack_kernel,
        [shape(CAP, wide, BF16)] * EXPERTS + [shape(count, LANES, F32)],
        [in_hbm(a) for a in (expert_ids.T, slots.T, tokens, router_weight.T)],
        in_specs=[hbm] * 4,
        scratch=[
            pltpu.VMEM(tokens.shape, BF16),
            pltpu.VMEM(router_weight.shape[::-1], BF16),
            pltpu.SMEM(slots.shape[::-1], jnp.int32),
            pltpu.SMEM(slots.shape[::-1], jnp.int32),
            pltpu.SemaphoreType.DMA((4,)),
        ],
    )
    arrived = [sends[0]] + [to_expert(sends[k], k) for k in range(1, EXPERTS)]
    size = EXPERTS * CAP
    gate_near, down_near = fetch([gate_weight, down_weight], sends[0])
    block_a = call(
        join_kernel,
        [shape(size, wide, BF16)],
        (*arrived, gate_near),
        in_specs=vmem(EXPERTS) + [pl.BlockSpec(memory_space=pl.ANY)],
    )[0]
    block_b = swap(block_a, "xi")

    got = {}
    for b, block in enumerate((block_a, block_b)):
        for sign in (1, -1):
            moving = block
            for d in range(1, REACH[b, sign] + 1):
                moving = along(moving, sign)
                got[b, sign, d] = moving
    parts = [[got[key] for key in keys] for keys in GROUPS]
    parts[0] = [block_a, block_b] + parts[0]
    rows = [size * len(part) for part in parts]
    near, far = [], []
    for group, part in enumerate(parts):
        near += call(
            functools.partial(stack_kernel, len(part)), [shape(rows[group], wide, BF16)], part
        )
        far.append(swap(near[group], "core"))

    units = gate_weight.shape[1]
    total_tokens = count * devices
    scale = EXPERTS / (2.0 * total_tokens * total_tokens)

    groups = len(GROUPS)
    outs = pl.pallas_call(
        functools.partial(expert_kernel, scale, groups),
        out_shape=[shape(n, width, dtype) for dtype in (F32, BF16) for n in rows]
        + [shape(1, 1, F32)],
        in_specs=vmem(2 * groups + 2) + [hbm],
        out_specs=vmem(2 * groups + 1),
        scratch_shapes=[
            pltpu.VMEM((2 * sum(rows), width), BF16),
            pltpu.VMEM((2 * sum(rows), units), BF16),
            pltpu.VMEM((width, units), BF16),
            pltpu.SemaphoreType.DMA((1,)),
        ],
        cost_estimate=pl.CostEstimate(
            flops=12 * sum(rows) * width * units, bytes_accessed=9_000_000, transcendentals=0
        ),
        compiler_params=pltpu.CompilerParams(vmem_limit_bytes=12 << 20),
    )(*near, *far, gate_near, down_near, in_hbm(up_weight))
    kept, sent = outs[:groups], outs[groups : 2 * groups]
    balance = outs[2 * groups].reshape(1)
    crossed = {}
    for group, value in reversed(list(enumerate(sent))):
        crossed[group] = swap(value, "core")

    moving = {}
    for group in reversed(range(len(GROUPS))):
        for d in sorted({key[2] for key in GROUPS[group]}, reverse=True):
            for b, sign in REACH:
                key = (b, sign, d)
                if key not in GROUPS[group]:
                    continue
                start = size * (GROUPS[group].index(key) + (2 if group == 0 else 0))
                came = [moving[b, sign]] if (b, sign) in moving else []
                value = call(
                    functools.partial(add_kernel, start),
                    [shape(size, width, BF16)],
                    [kept[group], crossed[group]] + came,
                )[0]
                moving[b, sign] = along(value, -sign)
    sums = []
    for b, dtype in ((1, BF16), (0, F32)):
        sums += call(
            functools.partial(add_kernel, b * size),
            [shape(size, width, dtype)],
            (kept[0], crossed[0], moving[b, 1], moving[b, -1]),
        )
    pieces = call(
        part_kernel,
        [shape(CAP, width, F32)] + [shape(CAP, width, BF16)] * 3,
        (sums[1], swap(sums[0], "xi")),
    )
    returned = [pieces[0]] + [to_expert(pieces[k], -k) for k in range(1, EXPERTS)]
    mixed_rows = call(mix_kernel, [shape(count, width, BF16)], (weights, *returned))[0]
    return (mixed_rows, balance)


def solution(mesh):
    split = Mesh(
        mesh.devices.reshape(mesh.shape["groups"], EXPERTS, PAIR, RING, CORES),
        GROUPS_EXPERT,
    )
    placed = (
        P(GROUPS_EXPERT, None),
        P("groups", None),
        P(GROUPS_EXPERT, None),
        P(GROUPS_EXPERT, None),
        P(None, EXPERT),
        P(None, EXPERT),
        P(EXPERT, None),
    )

    return jax.shard_map(
        local,
        mesh=split,
        in_specs=placed,
        out_specs=(P(GROUPS_EXPERT, None), P("groups")),
        check_vma=False,
    )
```

```python
import functools

import jax
import jax.numpy as jnp
from jax import lax
from jax.experimental import pallas as pl
from jax.experimental.pallas import tpu as pltpu
from jax.sharding import Mesh
from jax.sharding import PartitionSpec as P


EXPERTS = 4
CAP = 2
PAIR, RING, CORES = 2, 8, 2
LANES = 128
EXPERT = ("xo", "xi", "y", "core")
GROUPS_EXPERT = ("groups",) + EXPERT
F32, BF16 = jnp.float32, jnp.bfloat16
HALF = RING // 2
REACH = {(0, 1): HALF, (0, -1): HALF - 1, (1, 1): HALF - 1, (1, -1): HALF}
GROUPS = [
    [(b, sign, d) for d in distances for b in (0, 1) for sign in (1, -1) if d <= REACH[b, sign]]
    for distances in ((1,), (2,), (3,), (4,))
]


def vmem(count):
    return [pl.BlockSpec(memory_space=pltpu.VMEM)] * count


def call(kernel, outs, args, flops=200_000, in_specs=None, scratch=()):
    size = 1_000_000
    return pl.pallas_call(
        kernel,
        out_shape=outs,
        in_specs=in_specs or vmem(len(args)),
        out_specs=vmem(len(outs)),
        scratch_shapes=list(scratch),
        cost_estimate=pl.CostEstimate(flops=flops, bytes_accessed=size, transcendentals=0),
        compiler_params=pltpu.CompilerParams(vmem_limit_bytes=4 << 20),
    )(*args)


def shape(rows, width, dtype):
    return jax.ShapeDtypeStruct((rows, width), dtype)


def column_of(scalars, count):
    row = lax.broadcasted_iota(jnp.int32, (count, 1), 0)
    value = jnp.zeros((count, 1), jnp.int32)
    for t, scalar in enumerate(scalars):
        value = jnp.where(row == t, scalar, value)
    return value


def pack_kernel(
    ids_hbm,
    slots_hbm,
    tok_hbm,
    router_hbm,
    own,
    s1,
    s2,
    s3,
    cw_ref,
    tok_ref,
    router_ref,
    ids_s,
    slots_s,
    sems,
):
    copies = [
        pltpu.make_async_copy(tok_hbm, tok_ref, sems.at[0]),
        pltpu.make_async_copy(router_hbm, router_ref, sems.at[1]),
        pltpu.make_async_copy(ids_hbm, ids_s, sems.at[2]),
        pltpu.make_async_copy(slots_hbm, slots_s, sems.at[3]),
    ]
    for copy in copies:
        copy.start()
    here = lax.axis_index("xo")
    count, width = tok_ref.shape
    for copy in copies:
        copy.wait()
    ids = [column_of([ids_s[k, t] for t in range(count)], count) for k in range(2)]
    slots = [column_of([slots_s[k, t] for t in range(count)], count) for k in range(2)]
    tok = tok_ref[...].astype(F32)
    router = router_ref[...].astype(F32)
    logits = [
        jnp.sum(tok * router[e : e + 1, :], axis=1, keepdims=True) for e in range(EXPERTS)
    ]
    top = jnp.maximum(jnp.maximum(logits[0], logits[1]), jnp.maximum(logits[2], logits[3]))
    raised = [jnp.exp(v - top) for v in logits]
    inverse = 1.0 / (raised[0] + raised[1] + raised[2] + raised[3])
    lane = lax.broadcasted_iota(jnp.int32, (1, LANES), 1)
    count_row = jnp.zeros((1, LANES), F32)
    prob_row = jnp.zeros((1, LANES), F32)
    for e in range(EXPERTS):
        named = jnp.sum(
            (ids[0] == e).astype(F32) + (ids[1] == e).astype(F32), axis=0, keepdims=True
        )
        prob = jnp.sum(raised[e] * inverse, axis=0, keepdims=True)
        high = prob.astype(BF16).astype(F32)
        count_row = jnp.where((lane == e) | (lane == e + EXPERTS), named, count_row)
        prob_row = jnp.where(lane == e, high, prob_row)
        prob_row = jnp.where(lane == e + EXPERTS, prob - high, prob_row)
    statistic = jnp.concatenate([count_row, prob_row], axis=0).astype(BF16)
    chosen = []
    for k in range(2):
        picked = jnp.zeros_like(logits[0])
        for e in range(EXPERTS):
            picked = jnp.where(ids[k] == e, logits[e], picked)
        chosen.append(picked)
    top = jnp.maximum(chosen[0], chosen[1])
    chosen = [jnp.exp(v - top) for v in chosen]
    total = chosen[0] + chosen[1]
    gates = [v / total for v in chosen]
    lane = lax.broadcasted_iota(jnp.int32, (count, LANES), 1)
    weights = jnp.zeros((count, LANES), F32)
    for j, out in enumerate((own, s1, s2, s3)):
        expert = lax.rem(here + j, EXPERTS)
        rows = []
        for s in range(CAP):
            row = jnp.zeros((1, width), F32)
            for t in range(count):
                hit = ((ids_s[0, t] == expert) & (slots_s[0, t] == s)) | (
                    (ids_s[1, t] == expert) & (slots_s[1, t] == s)
                )
                row = jnp.where(hit, tok[t : t + 1, :], row)
            rows.append(row)
            column = jnp.zeros((count, 1), F32)
            for k in range(2):
                match = (ids[k] == expert) & (slots[k] == s)
                column = jnp.where(match, gates[k], column)
            weights = jnp.where(lane == j * CAP + s, column, weights)
        out[:, :width] = jnp.concatenate(rows, axis=0).astype(BF16)
        out[:, width:] = statistic
    cw_ref[...] = weights


def in_hbm(value):
    return pltpu.with_memory_space_constraint(value, pltpu.HBM)


def join_kernel(own, r1, r2, r3, unread, out):
    out[...] = jnp.concatenate([ref[...].astype(F32) for ref in (own, r1, r2, r3)], axis=0).astype(
        out.dtype
    )


def stack_kernel(count, *refs):
    start = 0
    for ref in refs[:count]:
        refs[-1][start : start + ref.shape[0], :] = ref[...]
        start += ref.shape[0]


def expert_kernel(scale, groups, *refs):
    blocks, (gate, up, down) = refs[: 2 * groups], refs[2 * groups : 2 * groups + 3]
    refs = refs[2 * groups + 3 :]
    outs, balance_ref = refs[: 2 * groups], refs[2 * groups]
    x_ref, hidden_ref = refs[2 * groups + 1 :]
    width = down.shape[1]
    start = 0
    total = jnp.zeros((8, LANES), F32)
    for block in blocks:
        rows = block.shape[0]
        x_ref[start : start + rows, :] = block[:, :width]
        start += rows
        for n in range(0, rows, 8):
            total = total + block[n : n + 8, width:].astype(F32)
    parity = lax.broadcasted_iota(jnp.int32, total.shape, 0) % 2
    named = jnp.sum(jnp.where(parity == 0, total, 0.0), axis=0, keepdims=True)
    probs = jnp.sum(jnp.where(parity == 1, total, 0.0), axis=0, keepdims=True)
    balance_ref[...] = jnp.sum(named * probs, axis=1, keepdims=True) * scale

    gate_pre = jnp.dot(x_ref[...], gate[...], preferred_element_type=F32)
    up_pre = jnp.dot(x_ref[...], up[...], preferred_element_type=F32)
    hidden_ref[...] = (gate_pre * jax.nn.sigmoid(gate_pre) * up_pre).astype(BF16)
    tile = 512

    def lower(i, carry):
        at = pl.ds(pl.multiple_of(i * tile, tile), tile)
        value = jnp.dot(hidden_ref[...], down[:, at], preferred_element_type=F32)
        start = 0
        for out in outs:
            out[:, at] = value[start : start + out.shape[0], :].astype(out.dtype)
            start += out.shape[0]
        return carry

    lax.fori_loop(0, width // tile, lower, 0)


def fetch_kernel(*refs):
    count = (len(refs) - 2) // 2
    copies = [
        pltpu.make_async_copy(refs[n], refs[count + 1 + n], refs[-1].at[n]) for n in range(count)
    ]
    for copy in copies:
        copy.start()
    for copy in copies:
        copy.wait()


def fetch(weights, after):
    return pl.pallas_call(
        fetch_kernel,
        out_shape=[pltpu.VMEM(w.shape, w.dtype) for w in weights],
        in_specs=[pl.BlockSpec(memory_space=pltpu.HBM)] * len(weights)
        + [pl.BlockSpec(memory_space=pl.ANY)],
        out_specs=vmem(len(weights)),
        scratch_shapes=[pltpu.SemaphoreType.DMA((len(weights),))],
        cost_estimate=pl.CostEstimate(
            flops=1_000_000,
            bytes_accessed=sum(2 * w.size * w.dtype.itemsize for w in weights),
            transcendentals=0,
        ),
        compiler_params=pltpu.CompilerParams(vmem_limit_bytes=4 << 20),
    )(*[in_hbm(w) for w in weights], after)


def add_kernel(start, kept_ref, crossed_ref, *refs):
    out = refs[-1]
    at = slice(start, start + out.shape[0])
    value = kept_ref[at, :] + crossed_ref[at, :].astype(F32)
    for ref in refs[:-1]:
        value = value + ref[...].astype(F32)
    out[...] = value.astype(out.dtype)


def part_kernel(a_ref, came_ref, own, s1, s2, s3):
    total = a_ref[...] + came_ref[...].astype(F32)
    for j, out in enumerate((own, s1, s2, s3)):
        out[...] = total[j * CAP : (j + 1) * CAP].astype(out.dtype)


def mix_kernel(cw_ref, own, r1, r2, r3, out):
    weights = cw_ref[...]
    total = None
    for j, ref in enumerate((own, r1, r2, r3)):
        value = ref[...].astype(F32)
        for s in range(CAP):
            at = j * CAP + s
            term = weights[:, at : at + 1] * value[s : s + 1, :]
            total = term if total is None else total + term
    out[...] = total.astype(out.dtype)


def in_hbm(value):
    return pltpu.with_memory_space_constraint(value, pltpu.HBM)


def to_expert(value, step):
    return lax.ppermute(value, "xo", [(i, (i + step) % EXPERTS) for i in range(EXPERTS)])


def swap(value, axis):
    return lax.ppermute(value, axis, [(0, 1), (1, 0)])


def along(value, step):
    return lax.ppermute(value, "y", [(y, (y + step) % RING) for y in range(RING)])


def local(tokens, router_weight, expert_ids, slots, gate_weight, up_weight, down_weight):
    devices = lax.axis_size(EXPERT)
    count, width = tokens.shape
    wide = width + LANES
    hbm = pl.BlockSpec(memory_space=pltpu.HBM)
    *sends, weights = call(
        pack_kernel,
        [shape(CAP, wide, BF16)] * EXPERTS + [shape(count, LANES, F32)],
        [in_hbm(a) for a in (expert_ids.T, slots.T, tokens, router_weight.T)],
        in_specs=[hbm] * 4,
        scratch=[
            pltpu.VMEM(tokens.shape, BF16),
            pltpu.VMEM(router_weight.shape[::-1], BF16),
            pltpu.SMEM(slots.shape[::-1], jnp.int32),
            pltpu.SMEM(slots.shape[::-1], jnp.int32),
            pltpu.SemaphoreType.DMA((4,)),
        ],
    )
    arrived = [sends[0]] + [to_expert(sends[k], k) for k in range(1, EXPERTS)]
    size = EXPERTS * CAP
    gate_near, up_near, down_near = fetch([gate_weight, up_weight, down_weight], sends[0])
    block_a = call(
        join_kernel,
        [shape(size, wide, BF16)],
        (*arrived, gate_near),
        in_specs=vmem(EXPERTS) + [pl.BlockSpec(memory_space=pl.ANY)],
    )[0]
    block_b = swap(block_a, "xi")

    got = {}
    for b, block in enumerate((block_a, block_b)):
        for sign in (1, -1):
            moving = block
            for d in range(1, REACH[b, sign] + 1):
                moving = along(moving, sign)
                got[b, sign, d] = moving
    parts = [[got[key] for key in keys] for keys in GROUPS]
    parts[0] = [block_a, block_b] + parts[0]
    rows = [size * len(part) for part in parts]
    near, far = [], []
    for group, part in enumerate(parts):
        near += call(
            functools.partial(stack_kernel, len(part)), [shape(rows[group], wide, BF16)], part
        )
        far.append(swap(near[group], "core"))

    units = gate_weight.shape[1]
    total_tokens = count * devices
    scale = EXPERTS / (2.0 * total_tokens * total_tokens)

    groups = len(GROUPS)
    outs = pl.pallas_call(
        functools.partial(expert_kernel, scale, groups),
        out_shape=[shape(n, width, dtype) for dtype in (F32, BF16) for n in rows]
        + [shape(1, 1, F32)],
        in_specs=vmem(2 * groups + 3),
        out_specs=vmem(2 * groups + 1),
        scratch_shapes=[
            pltpu.VMEM((2 * sum(rows), width), BF16),
            pltpu.VMEM((2 * sum(rows), units), BF16),
        ],
        cost_estimate=pl.CostEstimate(
            flops=12 * sum(rows) * width * units, bytes_accessed=9_000_000, transcendentals=0
        ),
        compiler_params=pltpu.CompilerParams(vmem_limit_bytes=12 << 20),
    )(*near, *far, gate_near, up_near, down_near)
    kept, sent = outs[:groups], outs[groups : 2 * groups]
    balance = outs[2 * groups].reshape(1)
    crossed = {}
    for group, value in reversed(list(enumerate(sent))):
        crossed[group] = swap(value, "core")

    moving = {}
    for group in reversed(range(len(GROUPS))):
        for d in sorted({key[2] for key in GROUPS[group]}, reverse=True):
            for b, sign in REACH:
                key = (b, sign, d)
                if key not in GROUPS[group]:
                    continue
                start = size * (GROUPS[group].index(key) + (2 if group == 0 else 0))
                came = [moving[b, sign]] if (b, sign) in moving else []
                value = call(
                    functools.partial(add_kernel, start),
                    [shape(size, width, BF16)],
                    [kept[group], crossed[group]] + came,
                )[0]
                moving[b, sign] = along(value, -sign)
    sums = []
    for b, dtype in ((1, BF16), (0, F32)):
        sums += call(
            functools.partial(add_kernel, b * size),
            [shape(size, width, dtype)],
            (kept[0], crossed[0], moving[b, 1], moving[b, -1]),
        )
    pieces = call(
        part_kernel,
        [shape(CAP, width, F32)] + [shape(CAP, width, BF16)] * 3,
        (sums[1], swap(sums[0], "xi")),
    )
    returned = [pieces[0]] + [to_expert(pieces[k], -k) for k in range(1, EXPERTS)]
    mixed_rows = call(mix_kernel, [shape(count, width, BF16)], (weights, *returned))[0]
    return (mixed_rows, balance)


def solution(mesh):
    split = Mesh(
        mesh.devices.reshape(mesh.shape["groups"], EXPERTS, PAIR, RING, CORES),
        GROUPS_EXPERT,
    )
    placed = (
        P(GROUPS_EXPERT, None),
        P("groups", None),
        P(GROUPS_EXPERT, None),
        P(GROUPS_EXPERT, None),
        P(None, EXPERT),
        P(None, EXPERT),
        P(EXPERT, None),
    )

    return jax.shard_map(
        local,
        mesh=split,
        in_specs=placed,
        out_specs=(P(GROUPS_EXPERT, None), P("groups")),
        check_vma=False,
    )
```

```python
import functools

import jax
import jax.numpy as jnp
from jax import lax
from jax.experimental import pallas as pl
from jax.experimental.pallas import tpu as pltpu
from jax.sharding import Mesh
from jax.sharding import PartitionSpec as P


EXPERTS = 4
CAP = 2
PAIR, RING, CORES = 2, 8, 2
LANES = 128
EXPERT = ("xo", "xi", "y", "core")
GROUPS_EXPERT = ("groups",) + EXPERT
F32, BF16 = jnp.float32, jnp.bfloat16
HALF = RING // 2
REACH = {(0, 1): HALF, (0, -1): HALF - 1, (1, 1): HALF - 1, (1, -1): HALF}
GROUPS = [
    [(b, sign, d) for d in distances for b in (0, 1) for sign in (1, -1) if d <= REACH[b, sign]]
    for distances in ((1,), (2,), (3,), (4,))
]


def vmem(count):
    return [pl.BlockSpec(memory_space=pltpu.VMEM)] * count


def call(kernel, outs, args, flops=200_000, in_specs=None, scratch=()):
    size = 1_000_000
    return pl.pallas_call(
        kernel,
        out_shape=outs,
        in_specs=in_specs or vmem(len(args)),
        out_specs=vmem(len(outs)),
        scratch_shapes=list(scratch),
        cost_estimate=pl.CostEstimate(flops=flops, bytes_accessed=size, transcendentals=0),
        compiler_params=pltpu.CompilerParams(vmem_limit_bytes=4 << 20),
    )(*args)


def shape(rows, width, dtype):
    return jax.ShapeDtypeStruct((rows, width), dtype)


def column_of(scalars, count):
    row = lax.broadcasted_iota(jnp.int32, (count, 1), 0)
    value = jnp.zeros((count, 1), jnp.int32)
    for t, scalar in enumerate(scalars):
        value = jnp.where(row == t, scalar, value)
    return value


def pack_kernel(
    ids_hbm,
    slots_hbm,
    tok_hbm,
    router_hbm,
    out,
    cw_ref,
    tok_ref,
    router_ref,
    ids_s,
    slots_s,
    sems,
):
    copies = [
        pltpu.make_async_copy(tok_hbm, tok_ref, sems.at[0]),
        pltpu.make_async_copy(router_hbm, router_ref, sems.at[1]),
        pltpu.make_async_copy(ids_hbm, ids_s, sems.at[2]),
        pltpu.make_async_copy(slots_hbm, slots_s, sems.at[3]),
    ]
    for copy in copies:
        copy.start()
    count, width = tok_ref.shape
    for copy in copies:
        copy.wait()
    ids = [column_of([ids_s[k, t] for t in range(count)], count) for k in range(2)]
    slots = [column_of([slots_s[k, t] for t in range(count)], count) for k in range(2)]
    tok = tok_ref[...].astype(F32)
    router = router_ref[...].astype(F32)
    logits = [
        jnp.sum(tok * router[e : e + 1, :], axis=1, keepdims=True) for e in range(EXPERTS)
    ]
    top = jnp.maximum(jnp.maximum(logits[0], logits[1]), jnp.maximum(logits[2], logits[3]))
    raised = [jnp.exp(v - top) for v in logits]
    inverse = 1.0 / (raised[0] + raised[1] + raised[2] + raised[3])
    lane = lax.broadcasted_iota(jnp.int32, (1, LANES), 1)
    count_row = jnp.zeros((1, LANES), F32)
    prob_row = jnp.zeros((1, LANES), F32)
    for e in range(EXPERTS):
        named = jnp.sum(
            (ids[0] == e).astype(F32) + (ids[1] == e).astype(F32), axis=0, keepdims=True
        )
        prob = jnp.sum(raised[e] * inverse, axis=0, keepdims=True)
        high = prob.astype(BF16).astype(F32)
        count_row = jnp.where((lane == e) | (lane == e + EXPERTS), named, count_row)
        prob_row = jnp.where(lane == e, high, prob_row)
        prob_row = jnp.where(lane == e + EXPERTS, prob - high, prob_row)
    statistic = jnp.concatenate([count_row, prob_row], axis=0).astype(BF16)
    chosen = []
    for k in range(2):
        picked = jnp.zeros_like(logits[0])
        for e in range(EXPERTS):
            picked = jnp.where(ids[k] == e, logits[e], picked)
        chosen.append(picked)
    top = jnp.maximum(chosen[0], chosen[1])
    chosen = [jnp.exp(v - top) for v in chosen]
    total = chosen[0] + chosen[1]
    gates = [v / total for v in chosen]
    lane = lax.broadcasted_iota(jnp.int32, (count, LANES), 1)
    weights = jnp.zeros((count, LANES), F32)
    for expert in range(EXPERTS):
        rows = []
        for s in range(CAP):
            row = jnp.zeros((1, width), F32)
            for t in range(count):
                hit = ((ids_s[0, t] == expert) & (slots_s[0, t] == s)) | (
                    (ids_s[1, t] == expert) & (slots_s[1, t] == s)
                )
                row = jnp.where(hit, tok[t : t + 1, :], row)
            rows.append(row)
            column = jnp.zeros((count, 1), F32)
            for k in range(2):
                match = (ids[k] == expert) & (slots[k] == s)
                column = jnp.where(match, gates[k], column)
            weights = jnp.where(lane == expert * CAP + s, column, weights)
        rows = jnp.concatenate(rows, axis=0).astype(BF16)
        for column in range(PAIR):
            out[expert * PAIR + column, :, :width] = rows
            out[expert * PAIR + column, :, width:] = statistic
    cw_ref[...] = weights


def halves_kernel(rows_ref, unread, a_ref, b_ref):
    half = rows_ref.shape[0] // 2
    for n, out in enumerate((a_ref, b_ref)):
        rows = [rows_ref[n * half + i].astype(F32) for i in range(half)]
        out[...] = jnp.concatenate(rows, axis=0).astype(out.dtype)


def stack_kernel(count, *refs):
    start = 0
    for ref in refs[:count]:
        refs[-1][start : start + ref.shape[0], :] = ref[...]
        start += ref.shape[0]


def expert_kernel(scale, groups, *refs):
    blocks, (gate, up, down) = refs[: 2 * groups], refs[2 * groups : 2 * groups + 3]
    refs = refs[2 * groups + 3 :]
    outs, balance_ref = refs[: 2 * groups], refs[2 * groups]
    x_ref, hidden_ref = refs[2 * groups + 1 :]
    width = down.shape[1]
    start = 0
    total = jnp.zeros((8, LANES), F32)
    for block in blocks:
        rows = block.shape[0]
        x_ref[start : start + rows, :] = block[:, :width]
        start += rows
        for n in range(0, rows, 8):
            total = total + block[n : n + 8, width:].astype(F32)
    parity = lax.broadcasted_iota(jnp.int32, total.shape, 0) % 2
    named = jnp.sum(jnp.where(parity == 0, total, 0.0), axis=0, keepdims=True)
    probs = jnp.sum(jnp.where(parity == 1, total, 0.0), axis=0, keepdims=True)
    balance_ref[...] = jnp.sum(named * probs, axis=1, keepdims=True) * scale

    gate_pre = jnp.dot(x_ref[...], gate[...], preferred_element_type=F32)
    up_pre = jnp.dot(x_ref[...], up[...], preferred_element_type=F32)
    hidden_ref[...] = (gate_pre * jax.nn.sigmoid(gate_pre) * up_pre).astype(BF16)
    tile = 512

    def lower(i, carry):
        at = pl.ds(pl.multiple_of(i * tile, tile), tile)
        value = jnp.dot(hidden_ref[...], down[:, at], preferred_element_type=F32)
        start = 0
        for out in outs:
            out[:, at] = value[start : start + out.shape[0], :].astype(out.dtype)
            start += out.shape[0]
        return carry

    lax.fori_loop(0, width // tile, lower, 0)


def fetch_kernel(*refs):
    count = (len(refs) - 2) // 2
    copies = [
        pltpu.make_async_copy(refs[n], refs[count + 1 + n], refs[-1].at[n]) for n in range(count)
    ]
    for copy in copies:
        copy.start()
    for copy in copies:
        copy.wait()


def fetch(weights, after):
    return pl.pallas_call(
        fetch_kernel,
        out_shape=[pltpu.VMEM(w.shape, w.dtype) for w in weights],
        in_specs=[pl.BlockSpec(memory_space=pltpu.HBM)] * len(weights)
        + [pl.BlockSpec(memory_space=pl.ANY)],
        out_specs=vmem(len(weights)),
        scratch_shapes=[pltpu.SemaphoreType.DMA((len(weights),))],
        cost_estimate=pl.CostEstimate(
            flops=1_000_000,
            bytes_accessed=sum(2 * w.size * w.dtype.itemsize for w in weights),
            transcendentals=0,
        ),
        compiler_params=pltpu.CompilerParams(vmem_limit_bytes=4 << 20),
    )(*[in_hbm(w) for w in weights], after)


def add_kernel(start, kept_ref, crossed_ref, *refs):
    out = refs[-1]
    at = slice(start, start + out.shape[0])
    value = kept_ref[at, :] + crossed_ref[at, :].astype(F32)
    for ref in refs[:-1]:
        value = value + ref[...].astype(F32)
    out[...] = value.astype(out.dtype)


def last_kernel(kept_ref, crossed_ref, *refs):
    out = refs[-1]
    half = out.shape[0] // 2
    size = half * CAP
    for b in range(2):
        at = slice(b * size, (b + 1) * size)
        total = kept_ref[at, :] + crossed_ref[at, :].astype(F32)
        total = total + refs[2 * b][...].astype(F32) + refs[2 * b + 1][...].astype(F32)
        for n in range(half):
            out[b * half + n] = total[n * CAP : (n + 1) * CAP].astype(out.dtype)


def mix_kernel(cw_ref, rows_ref, out):
    weights = cw_ref[...]
    total = None
    for expert in range(EXPERTS):
        value = rows_ref[expert * PAIR].astype(F32) + rows_ref[expert * PAIR + 1].astype(F32)
        for s in range(CAP):
            at = expert * CAP + s
            term = weights[:, at : at + 1] * value[s : s + 1, :]
            total = term if total is None else total + term
    out[...] = total.astype(out.dtype)


def in_hbm(value):
    return pltpu.with_memory_space_constraint(value, pltpu.HBM)


def across(value):
    return lax.all_to_all(value, ("xo", "xi"), split_axis=0, concat_axis=0, tiled=True)


def swap(value, axis):
    return lax.ppermute(value, axis, [(0, 1), (1, 0)])


def along(value, step):
    return lax.ppermute(value, "y", [(y, (y + step) % RING) for y in range(RING)])


def local(tokens, router_weight, expert_ids, slots, gate_weight, up_weight, down_weight):
    devices = lax.axis_size(EXPERT)
    count, width = tokens.shape
    wide = width + LANES
    hbm = pl.BlockSpec(memory_space=pltpu.HBM)
    columns = EXPERTS * PAIR
    packed, weights = call(
        pack_kernel,
        [
            jax.ShapeDtypeStruct((columns, CAP, wide), BF16),
            shape(count, LANES, F32),
        ],
        [in_hbm(a) for a in (expert_ids.T, slots.T, tokens, router_weight.T)],
        in_specs=[hbm] * 4,
        scratch=[
            pltpu.VMEM(tokens.shape, BF16),
            pltpu.VMEM(router_weight.shape[::-1], BF16),
            pltpu.SMEM(slots.shape[::-1], jnp.int32),
            pltpu.SMEM(slots.shape[::-1], jnp.int32),
            pltpu.SemaphoreType.DMA((4,)),
        ],
    )
    gate_near, up_near, down_near = fetch([gate_weight, up_weight, down_weight], packed)
    size = columns * CAP // 2
    block_a, block_b = call(
        halves_kernel,
        [shape(size, wide, BF16)] * 2,
        (across(packed), gate_near),
        in_specs=vmem(1) + [pl.BlockSpec(memory_space=pl.ANY)],
    )

    got = {}
    for b, block in enumerate((block_a, block_b)):
        for sign in (1, -1):
            moving = block
            for d in range(1, REACH[b, sign] + 1):
                moving = along(moving, sign)
                got[b, sign, d] = moving
    parts = [[got[key] for key in keys] for keys in GROUPS]
    parts[0] = [block_a, block_b] + parts[0]
    rows = [size * len(part) for part in parts]
    near, far = [], []
    for group, part in enumerate(parts):
        near += call(
            functools.partial(stack_kernel, len(part)), [shape(rows[group], wide, BF16)], part
        )
        far.append(swap(near[group], "core"))

    units = gate_weight.shape[1]
    total_tokens = count * devices
    scale = EXPERTS / (2.0 * total_tokens * total_tokens)

    groups = len(GROUPS)
    outs = pl.pallas_call(
        functools.partial(expert_kernel, scale, groups),
        out_shape=[shape(n, width, dtype) for dtype in (F32, BF16) for n in rows]
        + [shape(1, 1, F32)],
        in_specs=vmem(2 * groups + 3),
        out_specs=vmem(2 * groups + 1),
        scratch_shapes=[
            pltpu.VMEM((2 * sum(rows), width), BF16),
            pltpu.VMEM((2 * sum(rows), units), BF16),
        ],
        cost_estimate=pl.CostEstimate(
            flops=12 * sum(rows) * width * units, bytes_accessed=9_000_000, transcendentals=0
        ),
        compiler_params=pltpu.CompilerParams(vmem_limit_bytes=12 << 20),
    )(*near, *far, gate_near, up_near, down_near)
    kept, sent = outs[:groups], outs[groups : 2 * groups]
    balance = outs[2 * groups].reshape(1)
    crossed = {}
    for group, value in reversed(list(enumerate(sent))):
        crossed[group] = swap(value, "core")

    moving = {}
    for group in reversed(range(len(GROUPS))):
        for d in sorted({key[2] for key in GROUPS[group]}, reverse=True):
            for b, sign in REACH:
                key = (b, sign, d)
                if key not in GROUPS[group]:
                    continue
                start = size * (GROUPS[group].index(key) + (2 if group == 0 else 0))
                came = [moving[b, sign]] if (b, sign) in moving else []
                value = call(
                    functools.partial(add_kernel, start),
                    [shape(size, width, BF16)],
                    [kept[group], crossed[group]] + came,
                )[0]
                moving[b, sign] = along(value, -sign)
    sums = call(
        last_kernel,
        [jax.ShapeDtypeStruct((columns, CAP, width), BF16)],
        (kept[0], crossed[0], *[moving[b, sign] for b in (0, 1) for sign in (1, -1)]),
    )[0]
    mixed_rows = call(mix_kernel, [shape(count, width, BF16)], (weights, across(sums)))[0]
    return (mixed_rows, balance)


def solution(mesh):
    split = Mesh(
        mesh.devices.reshape(mesh.shape["groups"], EXPERTS, PAIR, RING, CORES),
        GROUPS_EXPERT,
    )
    placed = (
        P(GROUPS_EXPERT, None),
        P("groups", None),
        P(GROUPS_EXPERT, None),
        P(GROUPS_EXPERT, None),
        P(None, EXPERT),
        P(None, EXPERT),
        P(EXPERT, None),
    )

    return jax.shard_map(
        local,
        mesh=split,
        in_specs=placed,
        out_specs=(P(GROUPS_EXPERT, None), P("groups")),
        check_vma=False,
    )
```

```python
import functools

import jax
import jax.numpy as jnp
from jax import lax
from jax.experimental import pallas as pl
from jax.experimental.pallas import tpu as pltpu
from jax.sharding import Mesh
from jax.sharding import PartitionSpec as P


EXPERTS = 4
CAP = 2
PAIR, RING, CORES = 2, 8, 2
LANES = 128
EXPERT = ("xo", "xi", "y", "core")
GROUPS_EXPERT = ("groups",) + EXPERT
F32, BF16 = jnp.float32, jnp.bfloat16
HALF = RING // 2
REACH = {(0, 1): HALF, (0, -1): HALF - 1, (1, 1): HALF - 1, (1, -1): HALF}
GROUPS = [
    [(b, sign, d) for d in distances for b in (0, 1) for sign in (1, -1) if d <= REACH[b, sign]]
    for distances in ((1,), (2,), (3,), (4,))
]


def vmem(count):
    return [pl.BlockSpec(memory_space=pltpu.VMEM)] * count


def call(kernel, outs, args, flops=200_000, in_specs=None, scratch=()):
    size = 1_000_000
    return pl.pallas_call(
        kernel,
        out_shape=outs,
        in_specs=in_specs or vmem(len(args)),
        out_specs=vmem(len(outs)),
        scratch_shapes=list(scratch),
        cost_estimate=pl.CostEstimate(flops=flops, bytes_accessed=size, transcendentals=0),
        compiler_params=pltpu.CompilerParams(vmem_limit_bytes=4 << 20),
    )(*args)


def shape(rows, width, dtype):
    return jax.ShapeDtypeStruct((rows, width), dtype)


def column_of(scalars, count):
    row = lax.broadcasted_iota(jnp.int32, (count, 1), 0)
    value = jnp.zeros((count, 1), jnp.int32)
    for t, scalar in enumerate(scalars):
        value = jnp.where(row == t, scalar, value)
    return value


def pack_kernel(
    ids_hbm,
    slots_hbm,
    tok_hbm,
    router_hbm,
    out,
    cw_ref,
    tok_ref,
    router_ref,
    ids_s,
    slots_s,
    sems,
):
    copies = [
        pltpu.make_async_copy(tok_hbm, tok_ref, sems.at[0]),
        pltpu.make_async_copy(router_hbm, router_ref, sems.at[1]),
        pltpu.make_async_copy(ids_hbm, ids_s, sems.at[2]),
        pltpu.make_async_copy(slots_hbm, slots_s, sems.at[3]),
    ]
    for copy in copies:
        copy.start()
    count, width = tok_ref.shape
    for copy in copies:
        copy.wait()
    ids = [column_of([ids_s[k, t] for t in range(count)], count) for k in range(2)]
    slots = [column_of([slots_s[k, t] for t in range(count)], count) for k in range(2)]
    tok = tok_ref[...].astype(F32)
    router = router_ref[...].astype(F32)
    logits = [
        jnp.sum(tok * router[e : e + 1, :], axis=1, keepdims=True) for e in range(EXPERTS)
    ]
    top = jnp.maximum(jnp.maximum(logits[0], logits[1]), jnp.maximum(logits[2], logits[3]))
    raised = [jnp.exp(v - top) for v in logits]
    inverse = 1.0 / (raised[0] + raised[1] + raised[2] + raised[3])
    lane = lax.broadcasted_iota(jnp.int32, (1, LANES), 1)
    count_row = jnp.zeros((1, LANES), F32)
    prob_row = jnp.zeros((1, LANES), F32)
    for e in range(EXPERTS):
        named = jnp.sum(
            (ids[0] == e).astype(F32) + (ids[1] == e).astype(F32), axis=0, keepdims=True
        )
        prob = jnp.sum(raised[e] * inverse, axis=0, keepdims=True)
        high = prob.astype(BF16).astype(F32)
        count_row = jnp.where((lane == e) | (lane == e + EXPERTS), named, count_row)
        prob_row = jnp.where(lane == e, high, prob_row)
        prob_row = jnp.where(lane == e + EXPERTS, prob - high, prob_row)
    statistic = jnp.concatenate([count_row, prob_row], axis=0).astype(BF16)
    chosen = []
    for k in range(2):
        picked = jnp.zeros_like(logits[0])
        for e in range(EXPERTS):
            picked = jnp.where(ids[k] == e, logits[e], picked)
        chosen.append(picked)
    top = jnp.maximum(chosen[0], chosen[1])
    chosen = [jnp.exp(v - top) for v in chosen]
    total = chosen[0] + chosen[1]
    gates = [v / total for v in chosen]
    lane = lax.broadcasted_iota(jnp.int32, (count, LANES), 1)
    weights = jnp.zeros((count, LANES), F32)
    for expert in range(EXPERTS):
        rows = []
        for s in range(CAP):
            row = jnp.zeros((1, width), F32)
            for t in range(count):
                hit = ((ids_s[0, t] == expert) & (slots_s[0, t] == s)) | (
                    (ids_s[1, t] == expert) & (slots_s[1, t] == s)
                )
                row = jnp.where(hit, tok[t : t + 1, :], row)
            rows.append(row)
            column = jnp.zeros((count, 1), F32)
            for k in range(2):
                match = (ids[k] == expert) & (slots[k] == s)
                column = jnp.where(match, gates[k], column)
            weights = jnp.where(lane == expert * CAP + s, column, weights)
        rows = jnp.concatenate(rows, axis=0).astype(BF16)
        for column in range(PAIR):
            out[expert * PAIR + column, :, :width] = rows
            out[expert * PAIR + column, :, width:] = statistic
    cw_ref[...] = weights


def halves_kernel(rows_ref, unread, a_ref, b_ref):
    half = rows_ref.shape[0] // 2
    for n, out in enumerate((a_ref, b_ref)):
        rows = [rows_ref[n * half + i].astype(F32) for i in range(half)]
        out[...] = jnp.concatenate(rows, axis=0).astype(out.dtype)


def stack_kernel(count, *refs):
    start = 0
    for ref in refs[:count]:
        refs[-1][start : start + ref.shape[0], :] = ref[...]
        start += ref.shape[0]


def expert_kernel(scale, groups, *refs):
    blocks, (gate, up, down) = refs[: 2 * groups], refs[2 * groups : 2 * groups + 3]
    refs = refs[2 * groups + 3 :]
    outs, balance_ref = refs[: 2 * groups], refs[2 * groups]
    x_ref, hidden_ref = refs[2 * groups + 1 :]
    width = down.shape[1]
    start = 0
    total = jnp.zeros((8, LANES), F32)
    for block in blocks:
        rows = block.shape[0]
        x_ref[start : start + rows, :] = block[:, :width]
        start += rows
        for n in range(0, rows, 8):
            total = total + block[n : n + 8, width:].astype(F32)
    parity = lax.broadcasted_iota(jnp.int32, total.shape, 0) % 2
    named = jnp.sum(jnp.where(parity == 0, total, 0.0), axis=0, keepdims=True)
    probs = jnp.sum(jnp.where(parity == 1, total, 0.0), axis=0, keepdims=True)
    balance_ref[...] = jnp.sum(named * probs, axis=1, keepdims=True) * scale

    gate_pre = jnp.dot(x_ref[...], gate[...], preferred_element_type=F32)
    up_pre = jnp.dot(x_ref[...], up[...], preferred_element_type=F32)
    hidden_ref[...] = (gate_pre * jax.nn.sigmoid(gate_pre) * up_pre).astype(BF16)
    tile = 512

    def lower(i, carry):
        at = pl.ds(pl.multiple_of(i * tile, tile), tile)
        value = jnp.dot(hidden_ref[...], down[:, at], preferred_element_type=F32)
        start = 0
        for out in outs:
            out[:, at] = value[start : start + out.shape[0], :].astype(out.dtype)
            start += out.shape[0]
        return carry

    lax.fori_loop(0, width // tile, lower, 0)


def fetch_kernel(*refs):
    count = (len(refs) - 2) // 2
    copies = [
        pltpu.make_async_copy(refs[n], refs[count + 1 + n], refs[-1].at[n]) for n in range(count)
    ]
    for copy in copies:
        copy.start()
    for copy in copies:
        copy.wait()


def fetch(weights, after):
    return pl.pallas_call(
        fetch_kernel,
        out_shape=[pltpu.VMEM(w.shape, w.dtype) for w in weights],
        in_specs=[pl.BlockSpec(memory_space=pltpu.HBM)] * len(weights)
        + [pl.BlockSpec(memory_space=pl.ANY)],
        out_specs=vmem(len(weights)),
        scratch_shapes=[pltpu.SemaphoreType.DMA((len(weights),))],
        cost_estimate=pl.CostEstimate(
            flops=1_000_000,
            bytes_accessed=sum(2 * w.size * w.dtype.itemsize for w in weights),
            transcendentals=0,
        ),
        compiler_params=pltpu.CompilerParams(vmem_limit_bytes=4 << 20),
    )(*[in_hbm(w) for w in weights], after)


def add_kernel(start, kept_ref, crossed_ref, *refs):
    out = refs[-1]
    at = slice(start, start + out.shape[0])
    value = kept_ref[at, :] + crossed_ref[at, :].astype(F32)
    for ref in refs[:-1]:
        value = value + ref[...].astype(F32)
    out[...] = value.astype(out.dtype)


def last_kernel(kept_ref, crossed_ref, *refs):
    out = refs[-1]
    half = out.shape[0] // 2
    size = half * CAP
    for b in range(2):
        at = slice(b * size, (b + 1) * size)
        total = kept_ref[at, :] + crossed_ref[at, :].astype(F32)
        total = total + refs[2 * b][...].astype(F32) + refs[2 * b + 1][...].astype(F32)
        for n in range(half):
            out[b * half + n] = total[n * CAP : (n + 1) * CAP].astype(out.dtype)


def mix_kernel(cw_ref, rows_ref, out):
    weights = cw_ref[...]
    total = None
    for expert in range(EXPERTS):
        value = rows_ref[expert * PAIR].astype(F32) + rows_ref[expert * PAIR + 1].astype(F32)
        for s in range(CAP):
            at = expert * CAP + s
            term = weights[:, at : at + 1] * value[s : s + 1, :]
            total = term if total is None else total + term
    out[...] = total.astype(out.dtype)


def in_hbm(value):
    return pltpu.with_memory_space_constraint(value, pltpu.HBM)


def across(value):
    return lax.all_to_all(value, ("xo", "xi"), split_axis=0, concat_axis=0, tiled=True)


def swap(value, axis):
    return lax.ppermute(value, axis, [(0, 1), (1, 0)])


def along(value, step):
    return lax.ppermute(value, "y", [(y, (y + step) % RING) for y in range(RING)])


def local(tokens, router_weight, expert_ids, slots, gate_weight, up_weight, down_weight):
    devices = lax.axis_size(EXPERT)
    count, width = tokens.shape
    wide = width + LANES
    hbm = pl.BlockSpec(memory_space=pltpu.HBM)
    columns = EXPERTS * PAIR
    packed, weights = call(
        pack_kernel,
        [
            jax.ShapeDtypeStruct((columns, CAP, wide), BF16),
            shape(count, LANES, F32),
        ],
        [in_hbm(a) for a in (expert_ids.T, slots.T, tokens, router_weight.T)],
        in_specs=[hbm] * 4,
        scratch=[
            pltpu.VMEM(tokens.shape, BF16),
            pltpu.VMEM(router_weight.shape[::-1], BF16),
            pltpu.SMEM(slots.shape[::-1], jnp.int32),
            pltpu.SMEM(slots.shape[::-1], jnp.int32),
            pltpu.SemaphoreType.DMA((4,)),
        ],
    )
    gate_near = fetch([gate_weight], packed)[0]
    size = columns * CAP // 2
    block_a, block_b = call(
        halves_kernel,
        [shape(size, wide, BF16)] * 2,
        (across(packed), gate_near),
        in_specs=vmem(1) + [pl.BlockSpec(memory_space=pl.ANY)],
    )

    got = {}
    for b, block in enumerate((block_a, block_b)):
        for sign in (1, -1):
            moving = block
            for d in range(1, REACH[b, sign] + 1):
                moving = along(moving, sign)
                got[b, sign, d] = moving
    parts = [[got[key] for key in keys] for keys in GROUPS]
    parts[0] = [block_a, block_b] + parts[0]
    rows = [size * len(part) for part in parts]
    near, far = [], []
    for group, part in enumerate(parts):
        behind = []
        if group == len(parts) - 1:
            up_near, down_near = fetch([up_weight, down_weight], near[-1])
            behind = [up_near]
        near += call(
            functools.partial(stack_kernel, len(part)),
            [shape(rows[group], wide, BF16)],
            part + behind,
            in_specs=vmem(len(part)) + [pl.BlockSpec(memory_space=pl.ANY)] * len(behind),
        )
        far.append(swap(near[group], "core"))

    units = gate_weight.shape[1]
    total_tokens = count * devices
    scale = EXPERTS / (2.0 * total_tokens * total_tokens)

    groups = len(GROUPS)
    outs = pl.pallas_call(
        functools.partial(expert_kernel, scale, groups),
        out_shape=[shape(n, width, dtype) for dtype in (F32, BF16) for n in rows]
        + [shape(1, 1, F32)],
        in_specs=vmem(2 * groups + 3),
        out_specs=vmem(2 * groups + 1),
        scratch_shapes=[
            pltpu.VMEM((2 * sum(rows), width), BF16),
            pltpu.VMEM((2 * sum(rows), units), BF16),
        ],
        cost_estimate=pl.CostEstimate(
            flops=12 * sum(rows) * width * units, bytes_accessed=9_000_000, transcendentals=0
        ),
        compiler_params=pltpu.CompilerParams(vmem_limit_bytes=12 << 20),
    )(*near, *far, gate_near, up_near, down_near)
    kept, sent = outs[:groups], outs[groups : 2 * groups]
    balance = outs[2 * groups].reshape(1)
    crossed = {}
    for group, value in reversed(list(enumerate(sent))):
        crossed[group] = swap(value, "core")

    moving = {}
    for group in reversed(range(len(GROUPS))):
        for d in sorted({key[2] for key in GROUPS[group]}, reverse=True):
            for b, sign in REACH:
                key = (b, sign, d)
                if key not in GROUPS[group]:
                    continue
                start = size * (GROUPS[group].index(key) + (2 if group == 0 else 0))
                came = [moving[b, sign]] if (b, sign) in moving else []
                value = call(
                    functools.partial(add_kernel, start),
                    [shape(size, width, BF16)],
                    [kept[group], crossed[group]] + came,
                )[0]
                moving[b, sign] = along(value, -sign)
    sums = call(
        last_kernel,
        [jax.ShapeDtypeStruct((columns, CAP, width), BF16)],
        (kept[0], crossed[0], *[moving[b, sign] for b in (0, 1) for sign in (1, -1)]),
    )[0]
    mixed_rows = call(mix_kernel, [shape(count, width, BF16)], (weights, across(sums)))[0]
    return (mixed_rows, balance)


def solution(mesh):
    split = Mesh(
        mesh.devices.reshape(mesh.shape["groups"], EXPERTS, PAIR, RING, CORES),
        GROUPS_EXPERT,
    )
    placed = (
        P(GROUPS_EXPERT, None),
        P("groups", None),
        P(GROUPS_EXPERT, None),
        P(GROUPS_EXPERT, None),
        P(None, EXPERT),
        P(None, EXPERT),
        P(EXPERT, None),
    )

    return jax.shard_map(
        local,
        mesh=split,
        in_specs=placed,
        out_specs=(P(GROUPS_EXPERT, None), P("groups")),
        check_vma=False,
    )
```

```python
import functools

import jax
import jax.numpy as jnp
from jax import lax
from jax.experimental import pallas as pl
from jax.experimental.pallas import tpu as pltpu
from jax.sharding import Mesh
from jax.sharding import PartitionSpec as P


EXPERTS = 4
CAP = 2
PAIR, RING, CORES = 2, 8, 2
LANES = 128
EXPERT = ("xo", "xi", "y", "core")
GROUPS_EXPERT = ("groups",) + EXPERT
F32, BF16 = jnp.float32, jnp.bfloat16
HALF = RING // 2
REACH = {(0, 1): HALF, (0, -1): HALF - 1, (1, 1): HALF - 1, (1, -1): HALF}
GROUPS = [
    [(b, sign, d) for d in distances for b in (0, 1) for sign in (1, -1) if d <= REACH[b, sign]]
    for distances in ((1,), (2,), (3,), (4,))
]


def vmem(count):
    return [pl.BlockSpec(memory_space=pltpu.VMEM)] * count


def call(kernel, outs, args, flops=200_000, in_specs=None, scratch=()):
    size = 1_000_000
    return pl.pallas_call(
        kernel,
        out_shape=outs,
        in_specs=in_specs or vmem(len(args)),
        out_specs=vmem(len(outs)),
        scratch_shapes=list(scratch),
        cost_estimate=pl.CostEstimate(flops=flops, bytes_accessed=size, transcendentals=0),
        compiler_params=pltpu.CompilerParams(vmem_limit_bytes=4 << 20),
    )(*args)


def shape(rows, width, dtype):
    return jax.ShapeDtypeStruct((rows, width), dtype)


def column_of(scalars, count):
    row = lax.broadcasted_iota(jnp.int32, (count, 1), 0)
    value = jnp.zeros((count, 1), jnp.int32)
    for t, scalar in enumerate(scalars):
        value = jnp.where(row == t, scalar, value)
    return value


def pack_kernel(
    ids_hbm,
    slots_hbm,
    tok_hbm,
    router_hbm,
    own,
    s1,
    s2,
    s3,
    cw_ref,
    tok_ref,
    router_ref,
    ids_s,
    slots_s,
    sems,
):
    copies = [
        pltpu.make_async_copy(tok_hbm, tok_ref, sems.at[0]),
        pltpu.make_async_copy(router_hbm, router_ref, sems.at[1]),
        pltpu.make_async_copy(ids_hbm, ids_s, sems.at[2]),
        pltpu.make_async_copy(slots_hbm, slots_s, sems.at[3]),
    ]
    for copy in copies:
        copy.start()
    here = lax.axis_index("xo")
    count, width = tok_ref.shape
    for copy in copies:
        copy.wait()
    ids = [column_of([ids_s[k, t] for t in range(count)], count) for k in range(2)]
    slots = [column_of([slots_s[k, t] for t in range(count)], count) for k in range(2)]
    tok = tok_ref[...].astype(F32)
    router = router_ref[...].astype(F32)
    logits = [
        jnp.sum(tok * router[e : e + 1, :], axis=1, keepdims=True) for e in range(EXPERTS)
    ]
    top = jnp.maximum(jnp.maximum(logits[0], logits[1]), jnp.maximum(logits[2], logits[3]))
    raised = [jnp.exp(v - top) for v in logits]
    inverse = 1.0 / (raised[0] + raised[1] + raised[2] + raised[3])
    lane = lax.broadcasted_iota(jnp.int32, (1, LANES), 1)
    count_row = jnp.zeros((1, LANES), F32)
    prob_row = jnp.zeros((1, LANES), F32)
    for e in range(EXPERTS):
        named = jnp.sum(
            (ids[0] == e).astype(F32) + (ids[1] == e).astype(F32), axis=0, keepdims=True
        )
        prob = jnp.sum(raised[e] * inverse, axis=0, keepdims=True)
        high = prob.astype(BF16).astype(F32)
        count_row = jnp.where((lane == e) | (lane == e + EXPERTS), named, count_row)
        prob_row = jnp.where(lane == e, high, prob_row)
        prob_row = jnp.where(lane == e + EXPERTS, prob - high, prob_row)
    statistic = jnp.concatenate([count_row, prob_row], axis=0).astype(BF16)
    chosen = []
    for k in range(2):
        picked = jnp.zeros_like(logits[0])
        for e in range(EXPERTS):
            picked = jnp.where(ids[k] == e, logits[e], picked)
        chosen.append(picked)
    top = jnp.maximum(chosen[0], chosen[1])
    chosen = [jnp.exp(v - top) for v in chosen]
    total = chosen[0] + chosen[1]
    gates = [v / total for v in chosen]
    lane = lax.broadcasted_iota(jnp.int32, (count, LANES), 1)
    weights = jnp.zeros((count, LANES), F32)
    for j, out in enumerate((own, s1, s2, s3)):
        expert = lax.rem(here + j, EXPERTS)
        rows = []
        for s in range(CAP):
            row = jnp.zeros((1, width), F32)
            for t in range(count):
                hit = ((ids_s[0, t] == expert) & (slots_s[0, t] == s)) | (
                    (ids_s[1, t] == expert) & (slots_s[1, t] == s)
                )
                row = jnp.where(hit, tok[t : t + 1, :], row)
            rows.append(row)
            column = jnp.zeros((count, 1), F32)
            for k in range(2):
                match = (ids[k] == expert) & (slots[k] == s)
                column = jnp.where(match, gates[k], column)
            weights = jnp.where(lane == expert * CAP + s, column, weights)
        out[:, :width] = jnp.concatenate(rows, axis=0).astype(BF16)
        out[:, width:] = statistic
    cw_ref[...] = weights


def join_kernel(own, r1, r2, r3, unread, out):
    out[...] = jnp.concatenate([ref[...].astype(F32) for ref in (own, r1, r2, r3)], axis=0).astype(
        out.dtype
    )


def stack_kernel(count, *refs):
    start = 0
    for ref in refs[:count]:
        refs[-1][start : start + ref.shape[0], :] = ref[...]
        start += ref.shape[0]


def expert_kernel(scale, groups, *refs):
    blocks, (gate, up, down) = refs[: 2 * groups], refs[2 * groups : 2 * groups + 3]
    refs = refs[2 * groups + 3 :]
    outs, balance_ref = refs[: 2 * groups], refs[2 * groups]
    x_ref, hidden_ref = refs[2 * groups + 1 :]
    width = down.shape[1]
    start = 0
    total = jnp.zeros((8, LANES), F32)
    for block in blocks:
        rows = block.shape[0]
        x_ref[start : start + rows, :] = block[:, :width]
        start += rows
        for n in range(0, rows, 8):
            total = total + block[n : n + 8, width:].astype(F32)
    parity = lax.broadcasted_iota(jnp.int32, total.shape, 0) % 2
    named = jnp.sum(jnp.where(parity == 0, total, 0.0), axis=0, keepdims=True)
    probs = jnp.sum(jnp.where(parity == 1, total, 0.0), axis=0, keepdims=True)
    balance_ref[...] = jnp.sum(named * probs, axis=1, keepdims=True) * scale

    gate_pre = jnp.dot(x_ref[...], gate[...], preferred_element_type=F32)
    up_pre = jnp.dot(x_ref[...], up[...], preferred_element_type=F32)
    hidden_ref[...] = (gate_pre * jax.nn.sigmoid(gate_pre) * up_pre).astype(BF16)
    tile = 512

    def lower(i, carry):
        at = pl.ds(pl.multiple_of(i * tile, tile), tile)
        value = jnp.dot(hidden_ref[...], down[:, at], preferred_element_type=F32)
        start = 0
        for out in outs:
            out[:, at] = value[start : start + out.shape[0], :].astype(out.dtype)
            start += out.shape[0]
        return carry

    lax.fori_loop(0, width // tile, lower, 0)


def fetch_kernel(*refs):
    count = (len(refs) - 2) // 2
    copies = [
        pltpu.make_async_copy(refs[n], refs[count + 1 + n], refs[-1].at[n]) for n in range(count)
    ]
    for copy in copies:
        copy.start()
    for copy in copies:
        copy.wait()


def fetch(weights, after):
    return pl.pallas_call(
        fetch_kernel,
        out_shape=[pltpu.VMEM(w.shape, w.dtype) for w in weights],
        in_specs=[pl.BlockSpec(memory_space=pltpu.HBM)] * len(weights)
        + [pl.BlockSpec(memory_space=pl.ANY)],
        out_specs=vmem(len(weights)),
        scratch_shapes=[pltpu.SemaphoreType.DMA((len(weights),))],
        cost_estimate=pl.CostEstimate(
            flops=1_000_000,
            bytes_accessed=sum(2 * w.size * w.dtype.itemsize for w in weights),
            transcendentals=0,
        ),
        compiler_params=pltpu.CompilerParams(vmem_limit_bytes=4 << 20),
    )(*[in_hbm(w) for w in weights], after)


def add_kernel(start, kept_ref, crossed_ref, *refs):
    out = refs[-1]
    at = slice(start, start + out.shape[0])
    value = kept_ref[at, :] + crossed_ref[at, :].astype(F32)
    for ref in refs[:-1]:
        value = value + ref[...].astype(F32)
    out[...] = value.astype(out.dtype)


def last_kernel(kept_ref, crossed_ref, *refs):
    out = refs[-1]
    here, column = lax.axis_index("xo"), lax.axis_index("xi")
    size = EXPERTS * CAP
    for b in range(PAIR):
        at = slice(b * size, (b + 1) * size)
        total = kept_ref[at, :] + crossed_ref[at, :].astype(F32)
        total = total + refs[2 * b][...].astype(F32) + refs[2 * b + 1][...].astype(F32)
        owner = column if b == 0 else 1 - column
        for j in range(EXPERTS):
            entry = lax.rem(here + EXPERTS - j, EXPERTS) * PAIR + owner
            out[entry] = total[j * CAP : (j + 1) * CAP].astype(out.dtype)


def mix_kernel(cw_ref, rows_ref, out):
    weights = cw_ref[...]
    total = None
    for expert in range(EXPERTS):
        value = rows_ref[expert * PAIR].astype(F32) + rows_ref[expert * PAIR + 1].astype(F32)
        for s in range(CAP):
            at = expert * CAP + s
            term = weights[:, at : at + 1] * value[s : s + 1, :]
            total = term if total is None else total + term
    out[...] = total.astype(out.dtype)


def in_hbm(value):
    return pltpu.with_memory_space_constraint(value, pltpu.HBM)


def to_expert(value, step):
    return lax.ppermute(value, "xo", [(i, (i + step) % EXPERTS) for i in range(EXPERTS)])


def across(value):
    return lax.all_to_all(value, ("xo", "xi"), split_axis=0, concat_axis=0, tiled=True)


def swap(value, axis):
    return lax.ppermute(value, axis, [(0, 1), (1, 0)])


def along(value, step):
    return lax.ppermute(value, "y", [(y, (y + step) % RING) for y in range(RING)])


def local(tokens, router_weight, expert_ids, slots, gate_weight, up_weight, down_weight):
    devices = lax.axis_size(EXPERT)
    count, width = tokens.shape
    wide = width + LANES
    hbm = pl.BlockSpec(memory_space=pltpu.HBM)
    *sends, weights = call(
        pack_kernel,
        [shape(CAP, wide, BF16)] * EXPERTS + [shape(count, LANES, F32)],
        [in_hbm(a) for a in (expert_ids.T, slots.T, tokens, router_weight.T)],
        in_specs=[hbm] * 4,
        scratch=[
            pltpu.VMEM(tokens.shape, BF16),
            pltpu.VMEM(router_weight.shape[::-1], BF16),
            pltpu.SMEM(slots.shape[::-1], jnp.int32),
            pltpu.SMEM(slots.shape[::-1], jnp.int32),
            pltpu.SemaphoreType.DMA((4,)),
        ],
    )
    arrived = [sends[0]] + [to_expert(sends[k], k) for k in range(1, EXPERTS)]
    size = EXPERTS * CAP
    gate_near, up_near, down_near = fetch([gate_weight, up_weight, down_weight], sends[0])
    block_a = call(
        join_kernel,
        [shape(size, wide, BF16)],
        (*arrived, gate_near),
        in_specs=vmem(EXPERTS) + [pl.BlockSpec(memory_space=pl.ANY)],
    )[0]
    block_b = swap(block_a, "xi")

    got = {}
    for b, block in enumerate((block_a, block_b)):
        for sign in (1, -1):
            moving = block
            for d in range(1, REACH[b, sign] + 1):
                moving = along(moving, sign)
                got[b, sign, d] = moving
    parts = [[got[key] for key in keys] for keys in GROUPS]
    parts[0] = [block_a, block_b] + parts[0]
    rows = [size * len(part) for part in parts]
    near, far = [], []
    for group, part in enumerate(parts):
        near += call(
            functools.partial(stack_kernel, len(part)), [shape(rows[group], wide, BF16)], part
        )
        far.append(swap(near[group], "core"))

    units = gate_weight.shape[1]
    total_tokens = count * devices
    scale = EXPERTS / (2.0 * total_tokens * total_tokens)

    groups = len(GROUPS)
    outs = pl.pallas_call(
        functools.partial(expert_kernel, scale, groups),
        out_shape=[shape(n, width, dtype) for dtype in (F32, BF16) for n in rows]
        + [shape(1, 1, F32)],
        in_specs=vmem(2 * groups + 3),
        out_specs=vmem(2 * groups + 1),
        scratch_shapes=[
            pltpu.VMEM((2 * sum(rows), width), BF16),
            pltpu.VMEM((2 * sum(rows), units), BF16),
        ],
        cost_estimate=pl.CostEstimate(
            flops=12 * sum(rows) * width * units, bytes_accessed=9_000_000, transcendentals=0
        ),
        compiler_params=pltpu.CompilerParams(vmem_limit_bytes=12 << 20),
    )(*near, *far, gate_near, up_near, down_near)
    kept, sent = outs[:groups], outs[groups : 2 * groups]
    balance = outs[2 * groups].reshape(1)
    crossed = {}
    for group, value in reversed(list(enumerate(sent))):
        crossed[group] = swap(value, "core")

    moving = {}
    for group in reversed(range(len(GROUPS))):
        for d in sorted({key[2] for key in GROUPS[group]}, reverse=True):
            for b, sign in REACH:
                key = (b, sign, d)
                if key not in GROUPS[group]:
                    continue
                start = size * (GROUPS[group].index(key) + (2 if group == 0 else 0))
                came = [moving[b, sign]] if (b, sign) in moving else []
                value = call(
                    functools.partial(add_kernel, start),
                    [shape(size, width, BF16)],
                    [kept[group], crossed[group]] + came,
                )[0]
                moving[b, sign] = along(value, -sign)
    sums = call(
        last_kernel,
        [jax.ShapeDtypeStruct((EXPERTS * PAIR, CAP, width), BF16)],
        (kept[0], crossed[0], *[moving[b, sign] for b in (0, 1) for sign in (1, -1)]),
    )[0]
    mixed_rows = call(mix_kernel, [shape(count, width, BF16)], (weights, across(sums)))[0]
    return (mixed_rows, balance)


def solution(mesh):
    split = Mesh(
        mesh.devices.reshape(mesh.shape["groups"], EXPERTS, PAIR, RING, CORES),
        GROUPS_EXPERT,
    )
    placed = (
        P(GROUPS_EXPERT, None),
        P("groups", None),
        P(GROUPS_EXPERT, None),
        P(GROUPS_EXPERT, None),
        P(None, EXPERT),
        P(None, EXPERT),
        P(EXPERT, None),
    )

    return jax.shard_map(
        local,
        mesh=split,
        in_specs=placed,
        out_specs=(P(GROUPS_EXPERT, None), P("groups")),
        check_vma=False,
    )
```

```python
import functools

import jax
import jax.numpy as jnp
from jax import lax
from jax.experimental import pallas as pl
from jax.experimental.pallas import tpu as pltpu
from jax.sharding import Mesh
from jax.sharding import PartitionSpec as P


EXPERTS = 4
CAP = 2
PAIR, RING, CORES = 2, 8, 2
LANES = 128
EXPERT = ("xo", "xi", "y", "core")
GROUPS_EXPERT = ("groups",) + EXPERT
F32, BF16 = jnp.float32, jnp.bfloat16
HALF = RING // 2
REACH = {(0, 1): HALF, (0, -1): HALF - 1, (1, 1): HALF - 1, (1, -1): HALF}
GROUPS = [
    [(b, sign, d) for d in distances for b in (0, 1) for sign in (1, -1) if d <= REACH[b, sign]]
    for distances in ((1,), (2,), (3,), (4,))
]


def vmem(count):
    return [pl.BlockSpec(memory_space=pltpu.VMEM)] * count


def call(kernel, outs, args, flops=200_000, in_specs=None, scratch=()):
    size = 1_000_000
    return pl.pallas_call(
        kernel,
        out_shape=outs,
        in_specs=in_specs or vmem(len(args)),
        out_specs=vmem(len(outs)),
        scratch_shapes=list(scratch),
        cost_estimate=pl.CostEstimate(flops=flops, bytes_accessed=size, transcendentals=0),
        compiler_params=pltpu.CompilerParams(vmem_limit_bytes=4 << 20),
    )(*args)


def shape(rows, width, dtype):
    return jax.ShapeDtypeStruct((rows, width), dtype)


def column_of(scalars, count):
    row = lax.broadcasted_iota(jnp.int32, (count, 1), 0)
    value = jnp.zeros((count, 1), jnp.int32)
    for t, scalar in enumerate(scalars):
        value = jnp.where(row == t, scalar, value)
    return value


def pack_kernel(
    ids_hbm,
    slots_hbm,
    tok_hbm,
    router_hbm,
    own,
    s1,
    s2,
    s3,
    cw_ref,
    tok_ref,
    router_ref,
    ids_s,
    slots_s,
    sems,
):
    copies = [
        pltpu.make_async_copy(tok_hbm, tok_ref, sems.at[0]),
        pltpu.make_async_copy(router_hbm, router_ref, sems.at[1]),
        pltpu.make_async_copy(ids_hbm, ids_s, sems.at[2]),
        pltpu.make_async_copy(slots_hbm, slots_s, sems.at[3]),
    ]
    for copy in copies:
        copy.start()
    here = lax.axis_index("xo")
    count, width = tok_ref.shape
    for copy in copies:
        copy.wait()
    ids = [column_of([ids_s[k, t] for t in range(count)], count) for k in range(2)]
    slots = [column_of([slots_s[k, t] for t in range(count)], count) for k in range(2)]
    tok = tok_ref[...].astype(F32)
    router = router_ref[...].astype(F32)
    logits = [
        jnp.sum(tok * router[e : e + 1, :], axis=1, keepdims=True) for e in range(EXPERTS)
    ]
    top = jnp.maximum(jnp.maximum(logits[0], logits[1]), jnp.maximum(logits[2], logits[3]))
    raised = [jnp.exp(v - top) for v in logits]
    inverse = 1.0 / (raised[0] + raised[1] + raised[2] + raised[3])
    lane = lax.broadcasted_iota(jnp.int32, (1, LANES), 1)
    count_row = jnp.zeros((1, LANES), F32)
    prob_row = jnp.zeros((1, LANES), F32)
    for e in range(EXPERTS):
        named = jnp.sum(
            (ids[0] == e).astype(F32) + (ids[1] == e).astype(F32), axis=0, keepdims=True
        )
        prob = jnp.sum(raised[e] * inverse, axis=0, keepdims=True)
        high = prob.astype(BF16).astype(F32)
        count_row = jnp.where((lane == e) | (lane == e + EXPERTS), named, count_row)
        prob_row = jnp.where(lane == e, high, prob_row)
        prob_row = jnp.where(lane == e + EXPERTS, prob - high, prob_row)
    statistic = jnp.concatenate([count_row, prob_row], axis=0).astype(BF16)
    chosen = []
    for k in range(2):
        picked = jnp.zeros_like(logits[0])
        for e in range(EXPERTS):
            picked = jnp.where(ids[k] == e, logits[e], picked)
        chosen.append(picked)
    top = jnp.maximum(chosen[0], chosen[1])
    chosen = [jnp.exp(v - top) for v in chosen]
    total = chosen[0] + chosen[1]
    gates = [v / total for v in chosen]
    lane = lax.broadcasted_iota(jnp.int32, (count, LANES), 1)
    weights = jnp.zeros((count, LANES), F32)
    for j, out in enumerate((own, s1, s2, s3)):
        expert = lax.rem(here + j, EXPERTS)
        rows = []
        for s in range(CAP):
            row = jnp.zeros((1, width), F32)
            for t in range(count):
                hit = ((ids_s[0, t] == expert) & (slots_s[0, t] == s)) | (
                    (ids_s[1, t] == expert) & (slots_s[1, t] == s)
                )
                row = jnp.where(hit, tok[t : t + 1, :], row)
            rows.append(row)
            column = jnp.zeros((count, 1), F32)
            for k in range(2):
                match = (ids[k] == expert) & (slots[k] == s)
                column = jnp.where(match, gates[k], column)
            weights = jnp.where(lane == j * CAP + s, column, weights)
        out[:, :width] = jnp.concatenate(rows, axis=0).astype(BF16)
        out[:, width:] = statistic
    cw_ref[...] = weights


def join_kernel(own, r1, r2, r3, unread, out):
    out[...] = jnp.concatenate([ref[...].astype(F32) for ref in (own, r1, r2, r3)], axis=0).astype(
        out.dtype
    )


def stack_kernel(count, *refs):
    start = 0
    for ref in refs[:count]:
        refs[-1][start : start + ref.shape[0], :] = ref[...]
        start += ref.shape[0]


def expert_kernel(scale, groups, *refs):
    blocks, (gate, up, down) = refs[: 2 * groups], refs[2 * groups : 2 * groups + 3]
    refs = refs[2 * groups + 3 :]
    outs, balance_ref = refs[: 2 * groups], refs[2 * groups]
    x_ref, hidden_ref = refs[2 * groups + 1 :]
    width = down.shape[1]
    start = 0
    total = jnp.zeros((8, LANES), F32)
    for block in blocks:
        rows = block.shape[0]
        x_ref[start : start + rows, :] = block[:, :width]
        start += rows
        for n in range(0, rows, 8):
            total = total + block[n : n + 8, width:].astype(F32)
    parity = lax.broadcasted_iota(jnp.int32, total.shape, 0) % 2
    named = jnp.sum(jnp.where(parity == 0, total, 0.0), axis=0, keepdims=True)
    probs = jnp.sum(jnp.where(parity == 1, total, 0.0), axis=0, keepdims=True)
    balance_ref[...] = jnp.sum(named * probs, axis=1, keepdims=True) * scale

    gate_pre = jnp.dot(x_ref[...], gate[...], preferred_element_type=F32)
    up_pre = jnp.dot(x_ref[...], up[...], preferred_element_type=F32)
    hidden_ref[...] = (gate_pre * jax.nn.sigmoid(gate_pre) * up_pre).astype(BF16)
    tile = 512

    def lower(i, carry):
        at = pl.ds(pl.multiple_of(i * tile, tile), tile)
        value = jnp.dot(hidden_ref[...], down[:, at], preferred_element_type=F32)
        start = 0
        for out in outs:
            out[:, at] = value[start : start + out.shape[0], :].astype(out.dtype)
            start += out.shape[0]
        return carry

    lax.fori_loop(0, width // tile, lower, 0)


def fetch_kernel(*refs):
    count = (len(refs) - 2) // 2
    copies = [
        pltpu.make_async_copy(refs[n], refs[count + 1 + n], refs[-1].at[n]) for n in range(count)
    ]
    for copy in copies:
        copy.start()
    for copy in copies:
        copy.wait()


def fetch(weights, after):
    return pl.pallas_call(
        fetch_kernel,
        out_shape=[pltpu.VMEM(w.shape, w.dtype) for w in weights],
        in_specs=[pl.BlockSpec(memory_space=pltpu.HBM)] * len(weights)
        + [pl.BlockSpec(memory_space=pl.ANY)],
        out_specs=vmem(len(weights)),
        scratch_shapes=[pltpu.SemaphoreType.DMA((len(weights),))],
        cost_estimate=pl.CostEstimate(
            flops=1_000_000,
            bytes_accessed=sum(2 * w.size * w.dtype.itemsize for w in weights),
            transcendentals=0,
        ),
        compiler_params=pltpu.CompilerParams(vmem_limit_bytes=4 << 20),
    )(*[in_hbm(w) for w in weights], after)


def add_kernel(start, kept_ref, crossed_ref, *refs):
    out = refs[-1]
    at = slice(start, start + out.shape[0])
    value = kept_ref[at, :] + crossed_ref[at, :].astype(F32)
    for ref in refs[:-1]:
        value = value + ref[...].astype(F32)
    out[...] = value.astype(out.dtype)


def part_kernel(a_ref, came_ref, own, s1, s2, s3):
    total = a_ref[...] + came_ref[...].astype(F32)
    for j, out in enumerate((own, s1, s2, s3)):
        out[...] = total[j * CAP : (j + 1) * CAP].astype(out.dtype)


def mix_kernel(cw_ref, own, r1, r2, r3, out):
    weights = cw_ref[...]
    total = None
    for j, ref in enumerate((own, r1, r2, r3)):
        value = ref[...].astype(F32)
        for s in range(CAP):
            at = j * CAP + s
            term = weights[:, at : at + 1] * value[s : s + 1, :]
            total = term if total is None else total + term
    out[...] = total.astype(out.dtype)


def in_hbm(value):
    return pltpu.with_memory_space_constraint(value, pltpu.HBM)


def to_expert(value, step):
    return lax.ppermute(value, "xo", [(i, (i + step) % EXPERTS) for i in range(EXPERTS)])


def swap(value, axis):
    return lax.ppermute(value, axis, [(0, 1), (1, 0)])


def along(value, step):
    return lax.ppermute(value, "y", [(y, (y + step) % RING) for y in range(RING)])


def local(tokens, router_weight, expert_ids, slots, gate_weight, up_weight, down_weight):
    devices = lax.axis_size(EXPERT)
    count, width = tokens.shape
    wide = width + LANES
    hbm = pl.BlockSpec(memory_space=pltpu.HBM)
    *sends, weights = call(
        pack_kernel,
        [shape(CAP, wide, BF16)] * EXPERTS + [shape(count, LANES, F32)],
        [in_hbm(a) for a in (expert_ids.T, slots.T, tokens, router_weight.T)],
        in_specs=[hbm] * 4,
        scratch=[
            pltpu.VMEM(tokens.shape, BF16),
            pltpu.VMEM(router_weight.shape[::-1], BF16),
            pltpu.SMEM(slots.shape[::-1], jnp.int32),
            pltpu.SMEM(slots.shape[::-1], jnp.int32),
            pltpu.SemaphoreType.DMA((4,)),
        ],
    )
    arrived = [sends[0]] + [to_expert(sends[k], k) for k in range(1, EXPERTS)]
    size = EXPERTS * CAP
    gate_near = fetch([gate_weight], sends[0])[0]
    block_a = call(
        join_kernel,
        [shape(size, wide, BF16)],
        (*arrived, gate_near),
        in_specs=vmem(EXPERTS) + [pl.BlockSpec(memory_space=pl.ANY)],
    )[0]
    block_b = swap(block_a, "xi")

    got = {}
    for b, block in enumerate((block_a, block_b)):
        for sign in (1, -1):
            moving = block
            for d in range(1, REACH[b, sign] + 1):
                moving = along(moving, sign)
                got[b, sign, d] = moving
    parts = [[got[key] for key in keys] for keys in GROUPS]
    parts[0] = [block_a, block_b] + parts[0]
    rows = [size * len(part) for part in parts]
    near, far = [], []
    for group, part in enumerate(parts):
        behind = []
        if group == len(parts) - 1:
            up_near, down_near = fetch([up_weight, down_weight], near[-1])
            behind = [up_near]
        near += call(
            functools.partial(stack_kernel, len(part)),
            [shape(rows[group], wide, BF16)],
            part + behind,
            in_specs=vmem(len(part)) + [pl.BlockSpec(memory_space=pl.ANY)] * len(behind),
        )
        far.append(swap(near[group], "core"))

    units = gate_weight.shape[1]
    total_tokens = count * devices
    scale = EXPERTS / (2.0 * total_tokens * total_tokens)

    groups = len(GROUPS)
    outs = pl.pallas_call(
        functools.partial(expert_kernel, scale, groups),
        out_shape=[shape(n, width, dtype) for dtype in (F32, BF16) for n in rows]
        + [shape(1, 1, F32)],
        in_specs=vmem(2 * groups + 3),
        out_specs=vmem(2 * groups + 1),
        scratch_shapes=[
            pltpu.VMEM((2 * sum(rows), width), BF16),
            pltpu.VMEM((2 * sum(rows), units), BF16),
        ],
        cost_estimate=pl.CostEstimate(
            flops=12 * sum(rows) * width * units, bytes_accessed=9_000_000, transcendentals=0
        ),
        compiler_params=pltpu.CompilerParams(vmem_limit_bytes=12 << 20),
    )(*near, *far, gate_near, up_near, down_near)
    kept, sent = outs[:groups], outs[groups : 2 * groups]
    balance = outs[2 * groups].reshape(1)
    crossed = {}
    for group, value in reversed(list(enumerate(sent))):
        crossed[group] = swap(value, "core")

    moving = {}
    for group in reversed(range(len(GROUPS))):
        for d in sorted({key[2] for key in GROUPS[group]}, reverse=True):
            for b, sign in REACH:
                key = (b, sign, d)
                if key not in GROUPS[group]:
                    continue
                start = size * (GROUPS[group].index(key) + (2 if group == 0 else 0))
                came = [moving[b, sign]] if (b, sign) in moving else []
                value = call(
                    functools.partial(add_kernel, start),
                    [shape(size, width, BF16)],
                    [kept[group], crossed[group]] + came,
                )[0]
                moving[b, sign] = along(value, -sign)
    sums = []
    for b, dtype in ((1, BF16), (0, F32)):
        sums += call(
            functools.partial(add_kernel, b * size),
            [shape(size, width, dtype)],
            (kept[0], crossed[0], moving[b, 1], moving[b, -1]),
        )
    pieces = call(
        part_kernel,
        [shape(CAP, width, F32)] + [shape(CAP, width, BF16)] * 3,
        (sums[1], swap(sums[0], "xi")),
    )
    returned = [pieces[0]] + [to_expert(pieces[k], -k) for k in range(1, EXPERTS)]
    mixed_rows = call(mix_kernel, [shape(count, width, BF16)], (weights, *returned))[0]
    return (mixed_rows, balance)


def solution(mesh):
    split = Mesh(
        mesh.devices.reshape(mesh.shape["groups"], EXPERTS, PAIR, RING, CORES),
        GROUPS_EXPERT,
    )
    placed = (
        P(GROUPS_EXPERT, None),
        P("groups", None),
        P(GROUPS_EXPERT, None),
        P(GROUPS_EXPERT, None),
        P(None, EXPERT),
        P(None, EXPERT),
        P(EXPERT, None),
    )

    return jax.shard_map(
        local,
        mesh=split,
        in_specs=placed,
        out_specs=(P(GROUPS_EXPERT, None), P("groups")),
        check_vma=False,
    )
```
